128 devices in a mesh: tp: 16 (over z, y), dp: 8 (over x, core).
Axes of the slice: x: 4, y: 4, z: 4, core: 2. Of those that a mesh axis runs over, the one named last changes fastest.
Arguments:
- hidden: bfloat16 [8, 4096, 768], P('dp')
- residual: float32 [8, 4096, 768], P('dp')
- targets: int32 [8, 4096], P('dp')
- embedding: bfloat16 [50288, 768], P('tp')
- norm_w: float32 [768], replicated
Outputs:
- output 1: float32 [], replicated
- output 2: float32 [8, 4096, 768], P('dp')
- output 3: float32 [50288, 768], P('tp')
- output 4: float32 [768], replicated
All inputs are finite; a program needn't handle non-finite values.
Results may differ from the reference program's by a relative error of at most 0.001.
Values sent between devices are 32-bit elements.
A program may use at most 1 GiB of HBM per device.

```python
import jax
import jax.numpy as jnp
from jax import lax

BATCH = 8
SEQ = 4096
D = 768
VOCAB = 50288
NORM_EPS = 1e-5
HEAD_SCALE = 2.0
TOK_BLOCK = min(SEQ, 256)


def draw_targets(tgt_key):
    k_pick, k_head, k_wide = jax.random.split(tgt_key, 3)
    pick_wide = jax.random.randint(k_pick, (BATCH, SEQ), 0, 4)
    head_ids = jax.random.randint(k_head, (BATCH, SEQ), 0, VOCAB // 16)
    wide_ids = jax.random.randint(k_wide, (BATCH, SEQ), 0, VOCAB)
    targets = jnp.where(pick_wide == 0, wide_ids, head_ids)
    return targets.at[0, 0].set(VOCAB - 1).at[0, 1].set(0).astype(jnp.int32)


def setup_inputs(seed: int = 0) -> dict:
    root_key = jax.random.key(seed)
    k_hid, k_res, k_tgt, k_emb, k_norm = jax.random.split(root_key, 5)
    hidden = jax.random.normal(k_hid, (BATCH, SEQ, D), jnp.float32).astype(jnp.bfloat16)
    residual = jax.random.normal(k_res, (BATCH, SEQ, D), jnp.float32)
    targets = draw_targets(k_tgt)
    embedding = (jax.random.normal(k_emb, (VOCAB, D), jnp.float32) * (HEAD_SCALE * D ** -0.5)).astype(jnp.bfloat16)
    norm_w = 1.0 + 0.3 * jax.random.normal(k_norm, (D,), jnp.float32)
    return {'hidden': hidden, 'residual': residual, 'targets': targets, 'embedding': embedding, 'norm_w': norm_w}


def norm_apply(resid, norm_w):
    inv_rms = lax.rsqrt(jnp.mean(resid * resid, axis=-1, keepdims=True) + NORM_EPS)
    return resid * inv_rms * norm_w


def reference(hidden, residual, targets, embedding, norm_w):
    n_tok = BATCH * SEQ
    inv_n = 1.0 / n_tok
    n_blocks = n_tok // TOK_BLOCK
    resid_all = (residual + hidden.astype(jnp.float32)).reshape(n_blocks, TOK_BLOCK, D)
    tgt_all = targets.reshape(n_blocks, TOK_BLOCK)
    vocab_ids = jnp.arange(VOCAB, dtype=jnp.int32)

    def block_step(carry_acc, blk_inputs):
        grad_emb, grad_w, loss_sum = carry_acc
        resid_blk, tgt_blk = blk_inputs
        normed, norm_vjp = jax.vjp(norm_apply, resid_blk, norm_w)
        h_blk = normed.astype(jnp.bfloat16)
        logits = jnp.dot(h_blk, embedding.T, preferred_element_type=jnp.float32)
        row_max = jnp.max(logits, axis=-1, keepdims=True)
        exp_shift = jnp.exp(logits - row_max)
        sum_exp = jnp.sum(exp_shift, axis=-1, keepdims=True)
        is_target = vocab_ids[None, :] == tgt_blk[:, None]
        tgt_logit = jnp.sum(jnp.where(is_target, logits, 0.0), axis=-1)
        log_norm = row_max[:, 0] + jnp.log(sum_exp[:, 0])
        prob_rows = exp_shift / sum_exp
        dlogits = (jnp.where(is_target, prob_rows - 1.0, prob_rows) * inv_n).astype(jnp.bfloat16)
        grad_h = jnp.dot(dlogits, embedding, preferred_element_type=jnp.float32)
        grad_r, grad_wb = norm_vjp(grad_h)
        grad_emb = grad_emb + jnp.dot(dlogits.T, h_blk, preferred_element_type=jnp.float32)
        return (grad_emb, grad_w + grad_wb, loss_sum + jnp.sum(log_norm - tgt_logit)), grad_r

    init_acc = (jnp.zeros((VOCAB, D), jnp.float32), jnp.zeros((D,), jnp.float32), jnp.zeros((), jnp.float32))
    final_acc, grad_rows = lax.scan(block_step, init_acc, (resid_all, tgt_all))
    grad_emb, grad_w, loss_sum = final_acc
    return (loss_sum * inv_n, grad_rows.reshape(BATCH, SEQ, D), grad_emb, grad_w)
```

```python
import functools

import jax
import jax.numpy as jnp
from jax import lax
from jax.experimental import pallas as pl
from jax.experimental.pallas import tpu as pltpu
from jax.sharding import PartitionSpec as P

NORM_EPS = 1e-5
LANES = 128
MESH = pl.DeviceIdType.MESH
F32 = jnp.float32
BF16 = jnp.bfloat16
VMEM_BYTES = 67_043_328


def _dot(a, b, ca, cb):
    return lax.dot_general(a, b, (((ca,), (cb,)), ((), ())), preferred_element_type=F32)


def _logits_kernel(n_chunk, width, vocab, res_ref, hid_ref, tgt_ref, emb_ref, w_ref, h_ref, e_ref, mc_ref, st_ref):
    rows = res_ref.shape[0]
    resid = res_ref[...] + hid_ref[...].astype(F32)
    inv = lax.rsqrt(jnp.mean(resid * resid, axis=-1, keepdims=True) + NORM_EPS)
    h = (resid * inv * w_ref[...]).astype(BF16)
    h_ref[...] = h
    tgt = tgt_ref[:, 0:1]
    tgt = jnp.where((tgt >= 0) & (tgt < vocab), tgt, -1)
    lane = lax.broadcasted_iota(jnp.int32, (rows, width), 1)
    maxes, sums, picked = [], [], jnp.zeros((rows, 1), F32)
    for c in range(n_chunk):
        cols = pl.ds(c * width, width)
        logits = _dot(h, emb_ref[cols, :], 1, 1)
        if (c + 1) * width > vocab:
            real = lane < vocab - c * width
            peak = jnp.max(jnp.where(real, logits, -jnp.inf), axis=-1, keepdims=True)
            e = jnp.where(real, jnp.exp(logits - peak), 0.0)
        else:
            peak = jnp.max(logits, axis=-1, keepdims=True)
            e = jnp.exp(logits - peak)
        e_ref[:, cols] = e
        picked = picked + jnp.sum(jnp.where(lane == tgt - c * width, logits, 0.0), axis=-1, keepdims=True)
        maxes.append(peak)
        sums.append(jnp.sum(e, axis=-1, keepdims=True))
    top = functools.reduce(jnp.maximum, maxes)
    total = functools.reduce(jnp.add, [s * jnp.exp(m - top) for m, s in zip(maxes, sums)])
    slot = lax.broadcasted_iota(jnp.int32, (rows, LANES), 1)
    marks = jnp.where(slot == n_chunk, tgt.astype(F32), 0.0)
    for c in range(n_chunk):
        marks = jnp.where(slot == c, maxes[c], marks)
    mc_ref[...] = marks
    table = jnp.where(slot == 0, top, jnp.where(slot == 1, total, jnp.where(slot == 2, picked, 0.0)))
    n_tile = rows // LANES
    for j in range(n_tile):
        tile = table[j * LANES:(j + 1) * LANES, :].T
        row = pl.ds(pl.program_id(0) * n_tile + j, 1)
        for k in range(3):
            st_ref[k, row, :] = tile[k:k + 1, :]


def _forward(res, hid, tgt_cols, emb, w, vocab, n_chunk, block):
    n_tok, d = res.shape
    v_pad = emb.shape[0]
    return pl.pallas_call(
        functools.partial(_logits_kernel, n_chunk, v_pad // n_chunk, vocab),
        grid=(n_tok // block,),
        in_specs=[
            pl.BlockSpec((block, d), lambda i: (i, 0)),
            pl.BlockSpec((block, d), lambda i: (i, 0)),
            pl.BlockSpec((block, LANES), lambda i: (i, 0)),
            pl.BlockSpec((v_pad, d), lambda i: (0, 0)),
            pl.BlockSpec((1, d), lambda i: (0, 0)),
        ],
        out_specs=[
            pl.BlockSpec((block, d), lambda i: (i, 0)),
            pl.BlockSpec((block, v_pad), lambda i: (i, 0)),
            pl.BlockSpec((block, LANES), lambda i: (i, 0)),
            pl.BlockSpec((3, n_tok // LANES, LANES), lambda i: (0, 0, 0)),
        ],
        out_shape=[
            jax.ShapeDtypeStruct((n_tok, d), BF16),
            jax.ShapeDtypeStruct((n_tok, v_pad), F32),
            jax.ShapeDtypeStruct((n_tok, LANES), F32),
            jax.ShapeDtypeStruct((3, n_tok // LANES, LANES), F32),
        ],
        compiler_params=pltpu.CompilerParams(dimension_semantics=("arbitrary",), vmem_limit_bytes=60 * 2**20),
    )(res, hid, tgt_cols, emb, w)


def _backward_kernel(n_chunk, inv_n, n_tp,
                     st_ref, w_ref, e_hbm, h_hbm, mc_hbm, emb_hbm, res_hbm, hid_hbm,
                     gr_out, ge_out, small_out,
                     emb, ebuf, mcbuf, hbuf, gbuf, dh, ge, r1, r2, crecv, rx, sy, sz, st2, fin, gro, rown, hown, smb, smr,
                     emb_sem, e_sem, mc_sem, h_sem, own_sem, sy_s, sy_r, sz_s, sz_r, r1_s, r1_r, r2_s, r2_r,
                     ag2_s, ag2_r, ag1_s, ag1_r, out_sem, c_s, c_r, rx_s, rx_r, agx_s, agx_r, agc_s, agc_r, sm_s, sm_r):
    n_tok, d = dh.shape
    v_pad = emb.shape[0]
    width = v_pad // n_chunk
    br = n_tok // 16
    hb = LANES
    n_half = br // hb
    b2 = br // 4
    half_v = v_pad // 2
    bx = v_pad // 16

    tp = lax.axis_index('tp')
    dp = lax.axis_index('dp')
    y, z = lax.rem(tp, 4), lax.div(tp, 4)
    core, x = lax.rem(dp, 2), lax.div(dp, 2)

    def at_tp(dy, dz):
        return {'tp': lax.rem(z + dz, 4) * 4 + lax.rem(y + dy, 4)}

    def at_x(dx):
        return {'dp': lax.rem(x + dx, 4) * 2 + core}

    partner = {'dp': x * 2 + (1 - core)}

    def axis1(c, step):
        return at_tp(step * (1 - c), step * c)

    def axis2(c, step):
        return at_tp(step * c, step * (1 - c))

    def place1(c):
        return y * (1 - c) + z * c

    def place2(c):
        return z * (1 - c) + y * c

    def remote(src, dst, send, recv, device):
        return pltpu.make_async_remote_copy(src_ref=src, dst_ref=dst, send_sem=send, recv_sem=recv,
                                            device_id=device, device_id_type=MESH)

    STEP = (1, 3)

    def rows1(kind, c, s):
        i = place1(c)
        step = 1 + 2 * s
        chunk = lax.rem(i + jnp.where(kind == 0, 2, jnp.where(kind == 3, 0, step)), 4)
        half = jnp.where(kind == 1, 1 - s, s)
        return pl.multiple_of(c * (n_tok // 2) + chunk * (2 * br) + half * br, br)

    def piece_rows(idx):
        k = lax.div(idx, n_half)
        kind, c, s = lax.div(k, 4), lax.rem(lax.div(k, 2), 2), lax.rem(k, 2)
        return pl.multiple_of(rows1(kind, c, s) + lax.rem(idx, n_half) * hb, hb)

    def pieces(idx):
        slot = lax.rem(idx, 2)
        rows = pl.ds(piece_rows(idx), hb)
        return (pltpu.make_async_copy(e_hbm.at[rows, :], ebuf.at[slot], e_sem.at[slot]),
                pltpu.make_async_copy(mc_hbm.at[rows, :], mcbuf.at[slot], mc_sem.at[slot]))

    emb_copy = pltpu.make_async_copy(emb_hbm, emb, emb_sem)
    emb_copy.start()
    for idx in range(2):
        for cp in pieces(idx):
            cp.start()
    own_rows = []
    own_copies = []
    for c in range(2):
        rows = pl.multiple_of(c * (n_tok // 2) + place1(c) * (2 * br) + place2(c) * (2 * b2), 2 * b2)
        own_rows.append(rows)
        own_copies.append(pltpu.make_async_copy(res_hbm.at[pl.ds(rows, 2 * b2), :], rown.at[c], own_sem.at[c, 0]))
        own_copies.append(pltpu.make_async_copy(hid_hbm.at[pl.ds(rows, 2 * b2), :], hown.at[c], own_sem.at[c, 1]))
    for cp in own_copies:
        cp.start()

    barrier = pltpu.get_barrier_semaphore()
    for k in (1, 2, 3):
        for device in (at_tp(k, 0), at_tp(0, k), at_x(k)):
            pl.semaphore_signal(barrier, inc=1, device_id=device, device_id_type=MESH)
    pl.semaphore_signal(barrier, inc=1, device_id=partner, device_id_type=MESH)
    pl.semaphore_wait(barrier, 10)

    def combine(parts):
        top = functools.reduce(jnp.maximum, [p[0] for p in parts])
        total = functools.reduce(jnp.add, [p[1] * jnp.exp(p[0] - top) for p in parts])
        return top, total, functools.reduce(jnp.add, [p[2] for p in parts])

    y_copies = [remote(st_ref, sy.at[k], sy_s.at[k], sy_r.at[k], at_tp(k, 0)) for k in (1, 2, 3)]
    for cp in y_copies:
        cp.start()
    ge[...] = jnp.zeros_like(ge)
    for cp in y_copies:
        cp.wait_recv()
    first = combine([tuple(st_ref[k] for k in range(3))] + [tuple(sy[j, k] for k in range(3)) for j in (1, 2, 3)])
    for k in range(3):
        st2[k] = first[k]
    z_copies = [remote(st2, sz.at[k], sz_s.at[k], sz_r.at[k], at_tp(0, k)) for k in (1, 2, 3)]
    for cp in z_copies:
        cp.start()
    for cp in z_copies:
        cp.wait_recv()
    top, total, picked = combine([first] + [tuple(sz[j, k] for k in range(3)) for j in (1, 2, 3)])
    fin[0] = top
    fin[1] = inv_n / total
    loss = jnp.sum(top + jnp.log(total) - picked) * (inv_n / n_tp)
    emb_copy.wait()

    row_id = lax.broadcasted_iota(jnp.int32, (LANES, LANES), 0)
    lane = lax.broadcasted_iota(jnp.int32, (hb, width), 1)

    def r1_copy(kind, c, s):
        rows = pl.ds(rows1(kind, c, s), br)
        return remote(dh.at[rows, :], r1.at[c, s, kind], r1_s.at[c, s, kind], r1_r.at[c, s, kind], axis1(c, 1 + 2 * s))

    def h_copy(kind, j):
        c, s = lax.div(j, 2), lax.rem(j, 2)
        dst = pl.ds(pl.multiple_of(j * br, br), br)
        return pltpu.make_async_copy(h_hbm.at[pl.ds(rows1(kind, c, s), br), :], hbuf.at[dst, :], h_sem.at[j])

    def block(kind, j):
        c, s = lax.div(j, 2), lax.rem(j, 2)
        h_copy(kind, j).start()
        for hf in range(n_half):
            idx = (kind * 4 + j) * n_half + hf
            slot = lax.rem(idx, 2)
            for cp in pieces(idx):
                cp.wait()
            at = lax.div(piece_rows(idx), LANES)
            cols = jnp.where(row_id == 0, fin[0, pl.ds(at, 1), :], fin[1, pl.ds(at, 1), :]).T
            marks = mcbuf[slot]
            scale = jnp.exp(marks - cols[:, 0:1]) * cols[:, 1:2]
            tgt = marks[:, n_chunk:n_chunk + 1].astype(jnp.int32)
            dst = pl.ds(pl.multiple_of(j * br + hf * hb, hb), hb)
            for v in range(n_chunk):
                g = ebuf[slot, :, v * width:(v + 1) * width] * scale[:, v:v + 1]
                g = g - jnp.where(lane == tgt - v * width, inv_n, 0.0)
                gbuf[dst, v * width:(v + 1) * width] = g.astype(BF16)

            @pl.when(idx + 2 < 16 * n_half)
            def _():
                for cp in pieces(idx + 2):
                    cp.start()
        rows = pl.ds(rows1(kind, c, s), br)
        src = pl.ds(pl.multiple_of(j * br, br), br)
        dh[rows, :] = _dot(gbuf[src, :], emb[...], 1, 0)

        @pl.when(kind < 2)
        def _():
            r1_copy(kind, c, s).start()

        @pl.when(kind == 2)
        def _():
            r1_copy(0, c, s).wait_recv()
            dh[rows, :] = dh[rows, :] + r1[c, s, 0]
            r1_copy(2, c, s).start()

    def group(kind, carry):
        lax.fori_loop(0, 4, lambda j, carry: (block(kind, j), carry)[1], 0)
        for j in range(4):
            h_copy(kind, j).wait()

        def chunk(v, carry):
            cols = pl.ds(pl.multiple_of(v * width, width), width)
            ge[cols, :] = ge[cols, :] + _dot(gbuf[:, cols], hbuf[...], 0, 0)
            return carry

        return lax.fori_loop(0, n_chunk, chunk, carry)

    lax.fori_loop(0, 4, group, 0)

    mine = pl.multiple_of(core * half_v, half_v)
    other = pl.multiple_of((1 - core) * half_v, half_v)
    c_copy = remote(ge.at[pl.ds(other, half_v), :], crecv, c_s, c_r, partner)
    c_copy.start()
    c_copy.wait_recv()

    def add_core(i, carry):
        rows = pl.ds(pl.multiple_of(mine + i * bx, bx), bx)
        ge[rows, :] = ge[rows, :] + crecv[pl.ds(pl.multiple_of(i * bx, bx), bx), :]
        return carry

    lax.fori_loop(0, 8, add_core, 0)

    def rows_x(kind, s):
        chunk = lax.rem(x + (2 if kind == 0 else 0 if kind == 3 else STEP[s]), 4)
        return pl.multiple_of(mine + chunk * (2 * bx) + (1 - s if kind == 1 else s) * bx, bx)

    def rx_copy(kind, s):
        return remote(ge.at[pl.ds(rows_x(kind, s), bx), :], rx.at[s, kind], rx_s.at[s, kind], rx_r.at[s, kind], at_x(STEP[s]))

    for kind in (0, 1):
        for s in range(2):
            rx_copy(kind, s).start()

    for c in range(2):
        for s in range(2):
            r1_copy(1, c, s).wait_recv()
            r1_copy(2, c, s).wait_recv()
    for c in range(2):
        for half in range(2):
            rows = pl.ds(rows1(3, c, half), br)
            dh[rows, :] = dh[rows, :] + r1[c, half, 2] + r1[c, 1 - half, 1]

    def rows2(kind, c, s):
        i = place2(c)
        chunk = lax.rem(i + (2 if kind == 0 else 0 if kind == 3 else STEP[s]), 4)
        half = 1 - s if kind == 1 else s
        return pl.multiple_of(c * (n_tok // 2) + place1(c) * (2 * br) + chunk * (2 * b2) + half * b2, b2)

    def r2_copy(kind, c, s):
        rows = pl.ds(rows2(kind, c, s), b2)
        return remote(dh.at[rows, :], r2.at[c, s, kind], r2_s.at[c, s, kind], r2_r.at[c, s, kind], axis2(c, STEP[s]))

    for kind in (0, 1):
        for c in range(2):
            for s in range(2):
                r2_copy(kind, c, s).start()
    for c in range(2):
        for s in range(2):
            r2_copy(0, c, s).wait_recv()
            rows = pl.ds(rows2(2, c, s), b2)
            dh[rows, :] = dh[rows, :] + r2[c, s, 0]
            r2_copy(2, c, s).start()

    for s in range(2):
        rx_copy(0, s).wait_recv()
        rows = pl.ds(rows_x(2, s), bx)
        ge[rows, :] = ge[rows, :] + rx[s, 0]
        rx_copy(2, s).start()

    for cp in own_copies:
        cp.wait()
    for c in range(2):
        for s in range(2):
            r2_copy(1, c, s).wait_recv()
            r2_copy(2, c, s).wait_recv()
    w = w_ref[...]
    gw = jnp.zeros((1, d), F32)
    ag2_copies, out_copies = [], []
    for c in range(2):
        for half in range(2):
            rows = pl.ds(rows2(3, c, half), b2)
            grad_h = dh[rows, :] + r2[c, half, 2] + r2[c, 1 - half, 1]
            part = pl.ds(half * b2, b2)
            resid = rown[c, part, :] + hown[c, part, :].astype(F32)
            inv = lax.rsqrt(jnp.mean(resid * resid, axis=-1, keepdims=True) + NORM_EPS)
            normed = resid * inv
            dn = grad_h * w
            gro[c, part, :] = inv * (dn - normed * jnp.mean(dn * normed, axis=-1, keepdims=True))
            gw = gw + jnp.sum(grad_h * normed, axis=0, keepdims=True)
        at = pl.ds(own_rows[c], 2 * b2)
        for s in range(2):
            ag2_copies.append(remote(gro.at[c], gr_out.at[at, :], ag2_s.at[c, s, 0], ag2_r.at[c, s, 0], axis2(c, STEP[s])))
            ag2_copies[-1].start()
        out_copies.append(pltpu.make_async_copy(gro.at[c], gr_out.at[at, :], out_sem.at[c]))
        out_copies[-1].start()

    row8 = lax.broadcasted_iota(jnp.int32, (8, d), 0)
    small = jnp.where(row8 == 0, gw, jnp.where(row8 == 1, loss, 0.0))
    small_copies = []

    def small_start(phase, value):
        place = (y, z, x, core)[phase]
        smb[phase] = value
        smr[phase, place] = value
        devices = ([at_tp(k, 0) for k in (1, 2, 3)], [at_tp(0, k) for k in (1, 2, 3)], [at_x(k) for k in (1, 2, 3)], [partner])[phase]
        copies = [remote(smb.at[phase], smr.at[phase, place], sm_s.at[phase, k], sm_r.at[phase, k], device)
                  for k, device in enumerate(devices)]
        for cp in copies:
            cp.start()
        small_copies.extend(copies)
        return copies

    def small_finish(phase, copies):
        for cp in copies:
            cp.wait_recv()
        n = 2 if phase == 3 else 4
        return functools.reduce(jnp.add, [smr[phase, k] for k in range(n)])

    small_step = small_start(0, small)

    def gathered2(c, step):
        return pl.multiple_of(c * (n_tok // 2) + place1(c) * (2 * br) + lax.rem(place2(c) + step, 4) * (2 * b2), 2 * b2)

    fwd2 = []
    for c in range(2):
        for s in range(2):
            ag2_copies[2 * c + s].wait_recv()
            rows = pl.multiple_of(gathered2(c, STEP[1 - s]) + s * b2, b2)
            part = gr_out.at[pl.ds(rows, b2), :]
            fwd2.append(remote(part, part, ag2_s.at[c, s, 1], ag2_r.at[c, s, 1], axis2(c, STEP[s])))
            fwd2[-1].start()
    small_step = small_start(1, small_finish(0, small_step))
    ag1_copies = []
    for c in range(2):
        for s in range(2):
            fwd2[2 * c + s].wait_recv()
        out_copies[c].wait()
        part = gr_out.at[pl.ds(pl.multiple_of(c * (n_tok // 2) + place1(c) * (2 * br), 2 * br), 2 * br), :]
        for s in range(2):
            ag1_copies.append(remote(part, part, ag1_s.at[c, s, 0], ag1_r.at[c, s, 0], axis1(c, STEP[s])))
            ag1_copies[-1].start()
    small_step = small_start(2, small_finish(1, small_step))

    for s in range(2):
        rx_copy(1, s).wait_recv()
        rx_copy(2, s).wait_recv()
    for half in range(2):
        rows = pl.ds(rows_x(3, half), bx)
        ge[rows, :] = ge[rows, :] + rx[half, 2] + rx[1 - half, 1]

    def x_chunk(step):
        return pl.multiple_of(mine + lax.rem(x + step, 4) * (2 * bx), 2 * bx)

    at = pl.ds(x_chunk(0), 2 * bx)
    agx_copies = [remote(ge.at[at, :], ge_out.at[at, :], agx_s.at[s, 0], agx_r.at[s, 0], at_x(STEP[s])) for s in range(2)]
    for cp in agx_copies:
        cp.start()
    agc_copies = [remote(ge.at[at, :], ge_out.at[at, :], agc_s.at[0], agc_r.at[0], partner)]
    agc_copies[-1].start()
    out_copies.append(pltpu.make_async_copy(ge.at[at, :], ge_out.at[at, :], out_sem.at[2]))
    out_copies[-1].start()
    small_step = small_start(3, small_finish(2, small_step))
    small_out[...] = small_finish(3, small_step)

    fwdx = []
    for s in range(2):
        agx_copies[s].wait_recv()
        rows = pl.multiple_of(x_chunk(STEP[1 - s]) + s * bx, bx)
        part = ge_out.at[pl.ds(rows, bx), :]
        fwdx.append(remote(part, part, agx_s.at[s, 1], agx_r.at[s, 1], at_x(STEP[s])))
        fwdx[-1].start()
        whole = ge_out.at[pl.ds(x_chunk(STEP[1 - s]), 2 * bx), :]
        agc_copies.append(remote(whole, whole, agc_s.at[1 + s], agc_r.at[1 + s], partner))
        agc_copies[-1].start()

    fwd1 = []
    for c in range(2):
        for s in range(2):
            ag1_copies[2 * c + s].wait_recv()
            chunk = lax.rem(place1(c) + STEP[1 - s], 4)
            rows = pl.multiple_of(c * (n_tok // 2) + chunk * (2 * br) + s * br, br)
            part = gr_out.at[pl.ds(rows, br), :]
            fwd1.append(remote(part, part, ag1_s.at[c, s, 1], ag1_r.at[c, s, 1], axis1(c, STEP[s])))
            fwd1[-1].start()

    for s in range(2):
        fwdx[s].wait_recv()
        rows = pl.multiple_of(x_chunk(2) + s * bx, bx)
        part = ge_out.at[pl.ds(rows, bx), :]
        agc_copies.append(remote(part, part, agc_s.at[3 + s], agc_r.at[3 + s], partner))
        agc_copies[-1].start()

    for cp in agc_copies + fwd1:
        cp.wait_recv()
    out_copies[2].wait()

    def r1_sent(i, carry):
        r1_copy(lax.div(i, 4), lax.rem(lax.div(i, 2), 2), lax.rem(i, 2)).wait_send()
        return carry

    lax.fori_loop(0, 12, r1_sent, 0)
    for kind in range(3):
        for s in range(2):
            rx_copy(kind, s).wait_send()
            for c in range(2):
                r2_copy(kind, c, s).wait_send()
    for cp in y_copies + z_copies + [c_copy] + ag2_copies + fwd2 + ag1_copies + fwd1 + agx_copies + fwdx + agc_copies + small_copies:
        cp.wait_send()


def _backward(st, w, e, h, mc, emb, res, hid, n_chunk, inv_n, n_tp):
    n_tok, d = res.shape
    v_pad = emb.shape[0]
    br, bx = n_tok // 16, v_pad // 16
    b2 = br // 4
    tiles = n_tok // LANES
    dma = pltpu.SemaphoreType.DMA
    any_spec = pl.BlockSpec(memory_space=pl.ANY)
    vmem_spec = pl.BlockSpec(memory_space=pltpu.VMEM)
    flops = 4 * n_tok * v_pad * d
    return pl.pallas_call(
        functools.partial(_backward_kernel, n_chunk, inv_n, n_tp),
        in_specs=[vmem_spec, vmem_spec] + [any_spec] * 6,
        out_specs=[any_spec, any_spec, vmem_spec],
        out_shape=[
            jax.ShapeDtypeStruct((n_tok, d), F32),
            jax.ShapeDtypeStruct((v_pad, d), F32),
            jax.ShapeDtypeStruct((8, d), F32),
        ],
        scratch_shapes=[
            pltpu.VMEM((v_pad, d), BF16),
            pltpu.VMEM((2, LANES, v_pad), F32),
            pltpu.VMEM((2, LANES, LANES), F32),
            pltpu.VMEM((4 * br, d), BF16),
            pltpu.VMEM((4 * br, v_pad), BF16),
            pltpu.VMEM((n_tok, d), F32),
            pltpu.VMEM((v_pad, d), F32),
            pltpu.VMEM((2, 2, 3, br, d), F32),
            pltpu.VMEM((2, 2, 3, b2, d), F32),
            pltpu.VMEM((v_pad // 2, d), F32),
            pltpu.VMEM((2, 3, bx, d), F32),
            pltpu.VMEM((4, 3, tiles, LANES), F32),
            pltpu.VMEM((4, 3, tiles, LANES), F32),
            pltpu.VMEM((3, tiles, LANES), F32),
            pltpu.VMEM((2, tiles, LANES), F32),
            pltpu.VMEM((2, 2 * b2, d), F32),
            pltpu.VMEM((2, 2 * b2, d), F32),
            pltpu.VMEM((2, 2 * b2, d), BF16),
            pltpu.VMEM((4, 8, d), F32),
            pltpu.VMEM((4, 4, 8, d), F32),
            dma, dma((2,)), dma((2,)), dma((4,)), dma((2, 2)),
            dma((4,)), dma((4,)), dma((4,)), dma((4,)),
            dma((2, 2, 3)), dma((2, 2, 3)), dma((2, 2, 3)), dma((2, 2, 3)),
            dma((2, 2, 2)), dma((2, 2, 2)), dma((2, 2, 2)), dma((2, 2, 2)),
            dma((3,)), dma, dma, dma((2, 3)), dma((2, 3)), dma((2, 2)), dma((2, 2)),
            dma((5,)), dma((5,)), dma((4, 3)), dma((4, 3)),
        ],
        compiler_params=pltpu.CompilerParams(collective_id=0, has_side_effects=True, vmem_limit_bytes=VMEM_BYTES),
        cost_estimate=pl.CostEstimate(flops=flops, bytes_accessed=4 * n_tok * v_pad, transcendentals=0),
    )(st, w, e, h, mc, emb, res, hid)


def solution(mesh, n_chunk=5, width=640, block=512):
    def program(hidden, residual, targets, embedding, norm_w):
        inv_n = 1.0 / (hidden.shape[0] * hidden.shape[1])
        n_tp = mesh.shape['tp']

        def local_part(hid_loc, res_loc, tgt_loc, emb_loc, norm_vec):
            n_batch, n_seq, d = hid_loc.shape
            n_tok = n_batch * n_seq
            vocab = emb_loc.shape[0]
            v_pad = n_chunk * width
            hid, res = hid_loc.reshape(n_tok, d), res_loc.reshape(n_tok, d)
            ids = tgt_loc.reshape(n_tok) - lax.axis_index('tp') * vocab
            tgt_cols = jnp.broadcast_to(ids[:, None], (n_tok, LANES))
            emb = jnp.pad(emb_loc, ((0, v_pad - vocab), (0, 0)))
            w = norm_vec.reshape(1, d)
            h, e, mc, st = _forward(res, hid, tgt_cols, emb, w, vocab, n_chunk, block)
            gr, ge, small = _backward(st, w, e, h, mc, emb, res, hid, n_chunk, inv_n, n_tp)
            return small[1, 0], gr.reshape(n_batch, n_seq, d), ge[:vocab], small[0]

        sharded = jax.shard_map(
            local_part, mesh=mesh,
            in_specs=(P('dp', None, None), P('dp', None, None), P('dp', None), P('tp', None), P(None)),
            out_specs=(P(), P('dp', None, None), P('tp', None), P(None)),
            check_vma=False)
        return sharded(hidden, residual, targets, embedding, norm_w)

    return program
```

```python
import functools

import jax
import jax.numpy as jnp
from jax import lax
from jax.experimental import pallas as pl
from jax.experimental.pallas import tpu as pltpu
from jax.sharding import PartitionSpec as P

NORM_EPS = 1e-5
LANES = 128
MESH = pl.DeviceIdType.MESH
ROWS = 16
WIDE = 512
PAIR = (0, 1)
OTHERS = (1, 2, 3)
TWO = 2
RING = 4
F32 = jnp.float32
BF16 = jnp.bfloat16
VMEM_BYTES = 67_043_328
STEP = (1, 3)


class _Copy:
    def __init__(self, make, *args):
        self.make = functools.partial(make, *args)

    def start(self):
        self.make().start()

    def wait_recv(self):
        self.make().wait_recv()

    def wait_send(self):
        self.make().wait_send()


def _dot(a, b, ca, cb):
    return lax.dot_general(a, b, (((ca,), (cb,)), ((), ())), preferred_element_type=F32)


def _kernel(chunks, vocab, inv_n, n_tp,
            tgt_ref, w_ref, tail_ref, emb_hbm, res_hbm, hid_hbm,
            gr_out, ge_out, small_out, h_hbm, e_hbm, mc_hbm, g_hbm,
            emb, dh, ge, r1, r2, crecv, rx, st, sy, sz, st2, fin, rown, hown, losses, smb, smr,
            emb_sem, in_sem, l_sem, e_sem, gw_sem, gin_sem, hin_sem, own_sem, sy_s, sy_r, sz_s, sz_r, r1_s, r1_r, r2_s, r2_r,
            ag2_s, ag2_r, ag1_s, ag1_r, out_sem, c_s, c_r, rx_s, rx_r, agx_s, agx_r, agc_s, agc_r, sm_s, sm_r):
    n_tok, d = dh.shape
    v_pad = emb.shape[0]
    mw = (len(chunks) + 1) * LANES
    rb = 2 * LANES
    n_blk = n_tok // rb
    br = n_tok // 32
    b2 = br // 4
    dx = d // 2
    cx = v_pad // 4
    bx = cx // 2
    wx = ge.shape[1]
    ox = (cx // LANES) * LANES
    sl_rows = n_tok // 2

    tp = lax.axis_index('tp')
    dp = lax.axis_index('dp')
    y, z = lax.rem(tp, 4), lax.div(tp, 4)
    core, x = lax.rem(dp, 2), lax.div(dp, 2)

    def at_tp(dy, dz):
        return {'tp': lax.rem(z + dz, 4) * 4 + lax.rem(y + dy, 4)}

    def at_x(k):
        return {'dp': lax.rem(x + k, 4) * 2 + core}

    partner = {'dp': x * 2 + (1 - core)}

    def axis1(c, step):
        return at_tp(step * (1 - c), step * c)

    def axis2(c, step):
        return at_tp(step * c, step * (1 - c))

    def place1(c):
        return y * (1 - c) + z * c

    def place2(c):
        return z * (1 - c) + y * c

    def remote(src, dst, send, recv, device):
        return pltpu.make_async_remote_copy(src_ref=src, dst_ref=dst, send_sem=send, recv_sem=recv,
                                            device_id=device, device_id_type=MESH)

    def start(copies):
        for cp in copies:
            cp.start()

    def wait(copies):
        for cp in copies:
            cp.wait()

    sent = []

    def send(copies):
        start(copies)
        sent.extend(copies)
        return copies

    def recv(copies):
        for cp in copies:
            cp.wait_recv()

    barrier = pltpu.get_barrier_semaphore()
    for k in OTHERS:
        for device in (at_tp(k, 0), at_tp(0, k), at_x(k)):
            pl.semaphore_signal(barrier, inc=1, device_id=device, device_id_type=MESH)
    pl.semaphore_signal(barrier, inc=1, device_id=partner, device_id_type=MESH)

    whole = (vocab // 16) * 16
    tail = jnp.where(lax.broadcasted_iota(jnp.int32, (16, d), 0) < vocab - whole, tail_ref[...].astype(F32), 0.0)
    emb[whole:whole + 16, :] = tail.astype(BF16)
    emb[whole + 16:, :] = jnp.zeros((v_pad - whole - 16, d), BF16)
    emb_copy = pltpu.make_async_copy(emb_hbm.at[pl.ds(0, whole), :], emb.at[pl.ds(0, whole), :], emb_sem)
    emb_copy.start()
    own_rows, own_copies = [], []
    for sl in PAIR:
        for c in PAIR:
            rows = pl.multiple_of(sl * sl_rows + c * (sl_rows // 2) + place1(c) * (2 * br) + place2(c) * (2 * b2), 2 * b2)
            own_rows.append(rows)
            own_copies.append(pltpu.make_async_copy(res_hbm.at[pl.ds(rows, 2 * b2), :], rown.at[sl, c], own_sem.at[sl, c, 0]))
            own_copies.append(pltpu.make_async_copy(hid_hbm.at[pl.ds(rows, 2 * b2), :], hown.at[sl, c], own_sem.at[sl, c, 1]))

    def combine(parts):
        top = functools.reduce(jnp.maximum, [p[0] for p in parts])
        total = functools.reduce(jnp.add, [p[1] * jnp.exp(p[0] - top) for p in parts])
        return top, total, functools.reduce(jnp.add, [p[2] for p in parts])

    def stats_y(sl):
        return send([_Copy(lambda k: remote(st.at[sl], sy.at[sl, k], sy_s.at[sl, k], sy_r.at[sl, k], at_tp(k, 0)), k) for k in OTHERS])

    def stats_z(sl, copies):
        recv(copies)
        parts = combine([tuple(st[sl, k] for k in range(3))] + [tuple(sy[sl, j, k] for k in range(3)) for j in OTHERS])
        for k in range(3):
            st2[sl, k] = parts[k]
        return send([_Copy(lambda k: remote(st2.at[sl], sz.at[sl, k], sz_s.at[sl, k], sz_r.at[sl, k], at_tp(0, k)), k) for k in OTHERS])

    tiles_sl = sl_rows // LANES

    def stats_end(sl, copies):
        recv(copies)
        top, total, picked = combine([tuple(st2[sl, k] for k in range(3))] + [tuple(sz[sl, j, k] for k in range(3)) for j in OTHERS])
        fin[0, sl * tiles_sl:(sl + 1) * tiles_sl, :] = top
        fin[1, sl * tiles_sl:(sl + 1) * tiles_sl, :] = inv_n / total
        part = (top + jnp.log(total) - picked) * (inv_n / n_tp)
        losses[sl] = jnp.sum(jnp.sum(part, axis=0, keepdims=True), axis=1, keepdims=True) + jnp.zeros((8, LANES), F32)

    ahead = {}

    def block_rows(i):
        return pl.ds(pl.multiple_of(i * rb, rb), rb)

    def logits_stage(ebuf, mcbuf, rbuf, hbuf, hobuf, sums, picks, ids):
        def kept(v, first, size, k, width):
            return v, pl.ds((k // d) * rb + first, size), pl.ds(k % d, width)

        def loads(i):
            slot, rows = lax.rem(i, 2), block_rows(i)
            return (pltpu.make_async_copy(res_hbm.at[rows, :], rbuf.at[slot], in_sem.at[slot, 0, 0]),
                    pltpu.make_async_copy(hid_hbm.at[rows, :], hbuf.at[slot], in_sem.at[slot, 0, 1]))

        def stores(i):
            slot, rows = lax.rem(i, 2), block_rows(i)
            return (pltpu.make_async_copy(hobuf.at[slot], h_hbm.at[rows, :], l_sem.at[slot, 0, 0]),
                    pltpu.make_async_copy(ebuf.at[slot], e_hbm.at[rows, :], l_sem.at[slot, 0, 1]),
                    pltpu.make_async_copy(mcbuf.at[slot], mc_hbm.at[rows, :], l_sem.at[slot, 1, 0]))

        step = {}

        def one(i, carry):
            slot = lax.rem(i, 2)

            @pl.when(i == n_blk // 2)
            def _():
                pl.semaphore_wait(barrier, 10)
                step['y'] = stats_y(0)
                start(own_copies)

            @pl.when(i == 3 * n_blk // 4)
            def _():
                step['z'] = stats_z(0, step['y'])

            wait(loads(i))

            @pl.when(i >= 2)
            def _():
                wait(stores(i - 2))

            resid = rbuf[slot] + hbuf[slot].astype(F32)
            inv = lax.rsqrt(jnp.mean(resid * resid, axis=-1, keepdims=True) + NORM_EPS)
            h = (resid * inv * w_ref[...]).astype(BF16)
            hobuf[slot] = h
            for j in range(rb // LANES):
                row = (tgt_ref[pl.ds(i * (rb // LANES) + j, 1), :] - tp * vocab).astype(F32)
                col = jnp.broadcast_to(row, (LANES, LANES)).T
                ids[j * LANES:(j + 1) * LANES, :] = jnp.where((col >= 0) & (col < vocab), col, -1.0)
            mcbuf[slot, :, len(chunks) * LANES:] = ids[...]

            def finish(v):
                at = sum(chunks[:v])

                def some(r, carry):
                    first = pl.multiple_of(r * ROWS, ROWS)
                    rows = pl.ds(first, ROWS)
                    tgt = ids[rows, :].astype(jnp.int32)
                    tiles = [ge[kept(v, first, ROWS, k, LANES)] for k in range(0, chunks[v], LANES)]
                    pick = jnp.zeros((ROWS, LANES), F32)
                    for k, tile in enumerate(tiles):
                        pick = pick + jnp.where(lane == tgt - (at + k * LANES), tile, 0.0)
                    real = lane < vocab - (at + chunks[v] - LANES)
                    if at + chunks[v] > vocab:
                        top = functools.reduce(jnp.maximum, tiles[:-1] + [jnp.where(real, tiles[-1], -jnp.inf)])
                    else:
                        top = functools.reduce(jnp.maximum, tiles)
                    total = jnp.zeros((ROWS, LANES), F32)
                    for k, tile in enumerate(tiles):
                        e = jnp.exp(tile - top)
                        if at + (k + 1) * LANES > vocab:
                            e = jnp.where(real, e, 0.0)
                        ebuf[slot, rows, at + k * LANES:at + (k + 1) * LANES] = e
                        total = total + e
                    mcbuf[slot, rows, v * LANES:(v + 1) * LANES] = top
                    sums[v, rows, :] = total
                    picks[v, rows, :] = pick
                    return carry

                lax.fori_loop(0, rb // ROWS, some, 0, unroll=True)

            lane = lax.broadcasted_iota(jnp.int32, (ROWS, LANES), 1)
            at = 0
            for v, width in enumerate(chunks):
                for k in range(0, width, d):
                    part = min(d, width - k)
                    ge[kept(v, 0, rb, k, part)] = _dot(h, emb[at + k:at + k + part, :], 1, 1)
                if v:
                    finish(v - 1)
                at += width
            finish(len(chunks) - 1)
            maxes = [mcbuf[slot, :, v * LANES:(v + 1) * LANES] for v in range(len(chunks))]
            top = jnp.max(functools.reduce(jnp.maximum, maxes), axis=-1, keepdims=True)
            total = functools.reduce(jnp.add, [sums[v] * jnp.exp(m - top) for v, m in enumerate(maxes)])
            total = jnp.sum(total, axis=-1, keepdims=True)
            picked = jnp.sum(functools.reduce(jnp.add, [picks[v] for v in range(len(chunks))]), axis=-1, keepdims=True)
            lane = lax.broadcasted_iota(jnp.int32, (rb, LANES), 1)
            table = jnp.where(lane == 0, top, jnp.where(lane == 1, total, picked))
            sl = lax.div(i, n_blk // 2)
            for j in range(rb // LANES):
                tile = table[j * LANES:(j + 1) * LANES, :].T
                row = pl.ds((i - sl * (n_blk // 2)) * (rb // LANES) + j, 1)
                for k in range(3):
                    st[sl, k, row, :] = tile[k:k + 1, :]
            start(stores(i))

            @pl.when(i + 2 < n_blk)
            def _():
                start(loads(i + 2))

            return carry

        start(loads(0))
        start(loads(1))
        emb_copy.wait()
        lax.fori_loop(0, n_blk, one, 0)
        ahead['y'] = stats_y(1)
        wait(stores(n_blk - 2))
        wait(stores(n_blk - 1))
        stats_end(0, step['z'])

    def rows1(sl, kind, c, s):
        step = 1 + 2 * s
        chunk = lax.rem(place1(c) + jnp.where(kind == 0, 2, jnp.where(kind == 3, 0, step)), 4)
        half = jnp.where(kind == 1, 1 - s, s)
        return pl.multiple_of(sl * sl_rows + c * (sl_rows // 2) + chunk * (2 * br) + half * br, br)

    def r1_copy(sl, kind, c, s):
        rows = pl.ds(rows1(sl, kind, c, s), br)
        return remote(dh.at[rows, :], r1.at[sl, c, s, kind], r1_s.at[sl, c, s, kind], r1_r.at[sl, c, s, kind], axis1(c, 1 + 2 * s))

    def gradient_stage(ebuf, mcbuf, gbuf0, gbuf1, spread):
        gbufs = (gbuf0, gbuf1)
        row_id = lax.broadcasted_iota(jnp.int32, (LANES, LANES), 0)
        lane = lax.broadcasted_iota(jnp.int32, (ROWS, WIDE), 1)

        def piece(b, c, s):
            b = lax.rem(b, n_blk)
            return rows1(lax.div(b, 8), lax.rem(lax.div(b, 2), 4), c, s)

        def loads(b, c):
            out = []
            for s in PAIR:
                rows = pl.ds(piece(b, c, s), br)
                part = pl.ds(s * br, br)
                out.append(pltpu.make_async_copy(e_hbm.at[rows, :], ebuf.at[c, part, :], e_sem.at[c, s, 0]))
                out.append(pltpu.make_async_copy(mc_hbm.at[rows, :], mcbuf.at[c, part, :], e_sem.at[c, s, 1]))
            return out

        def stores(b, c):
            return [pltpu.make_async_copy(gbufs[c].at[pl.ds(s * br, br), :], g_hbm.at[pl.ds(piece(b, c, s), br), :], gw_sem.at[c, s, 0])
                    for s in PAIR]

        def prepare(b, c):
            for s in PAIR:
                at = lax.div(piece(b, c, s), LANES)
                cols = jnp.where(row_id == 0, fin[0, pl.ds(at, 1), :], fin[1, pl.ds(at, 1), :]).T
                part = slice(s * br, (s + 1) * br)
                for v in range(len(chunks)):
                    lanes = slice(v * LANES, (v + 1) * LANES)
                    spread[v, part, :] = jnp.exp(mcbuf[c, part, lanes] - cols[:, 0:1]) * cols[:, 1:2]

        def make_g(c, unroll=True):
            def some(r, carry):
                rows = pl.ds(pl.multiple_of(r * ROWS, ROWS), ROWS)
                tgt = mcbuf[c, rows, len(chunks) * LANES:].astype(jnp.int32)
                at = 0
                for v, width in enumerate(chunks):
                    scale = spread[v, rows, :]
                    for k in range(at, at + width, WIDE):
                        n = min(WIDE, at + width - k)
                        hit = lane[:, :n] == jnp.concatenate([tgt - k] * (n // LANES), axis=1)
                        g = ebuf[c, rows, k:k + n] * jnp.concatenate([scale] * (n // LANES), axis=1) - jnp.where(hit, inv_n, 0.0)
                        gbufs[c][rows, k:k + n] = g.astype(BF16)
                    at += width
                return carry

            lax.fori_loop(0, rb // ROWS, some, 0, unroll=unroll)

        def step(b, c):
            nb, nc = b + 1, 1 - c
            sl, kind = lax.div(b, 8), lax.rem(lax.div(b, 2), 4)
            wait(loads(nb, nc))

            @pl.when(nb >= 2)
            def _():
                wait(stores(nb - 2, nc))

            prepare(nb, nc)
            rows = [pl.ds(rows1(sl, kind, c, s), br) for s in PAIR]

            make_g(nc)
            value = _dot(gbufs[c][...], emb[...], 1, 0)
            for s in PAIR:
                dh[rows[s], :] = value[s * br:(s + 1) * br, :]

            @pl.when(nb < n_blk)
            def _():
                start(stores(nb, nc))

            @pl.when(nb + 2 <= n_blk)
            def _():
                start(loads(nb + 2, nc))

            @pl.when(kind < 2)
            def _():
                for s in PAIR:
                    r1_copy(sl, kind, c, s).start()

            @pl.when(kind == 2)
            def _():
                for s in PAIR:
                    r1_copy(sl, 0, c, s).wait_recv()
                    rows = pl.ds(rows1(sl, kind, c, s), br)
                    dh[rows, :] = dh[rows, :] + r1[sl, c, s, 0]
                    r1_copy(sl, 2, c, s).start()

        def pair(kk, carry):
            @pl.when(kk == 2)
            def _():
                stats_end(1, ahead['z'])

            step(2 * kk, 0)
            step(2 * kk + 1, 1)
            return carry

        start(loads(0, 0))
        start(loads(1, 1))
        wait(loads(0, 0))
        prepare(0, 0)
        make_g(0, False)
        start(stores(0, 0))
        start(loads(2, 0))
        ahead['z'] = stats_z(1, ahead['y'])
        lax.fori_loop(0, n_blk // 2, pair, 0)
        wait(stores(n_blk - 1, 1))

    def rows2(sl, kind, c, s):
        chunk = lax.rem(place2(c) + (2 if kind == 0 else 0 if kind == 3 else STEP[s]), 4)
        half = 1 - s if kind == 1 else s
        return pl.multiple_of(sl * sl_rows + c * (sl_rows // 2) + place1(c) * (2 * br) + chunk * (2 * b2) + half * b2, b2)

    def r2_copy(sl, kind, c, s):
        rows = pl.ds(rows2(sl, kind, c, s), b2)
        return remote(dh.at[rows, :], r2.at[sl, c, s, kind], r2_s.at[sl, c, s, kind], r2_r.at[sl, c, s, kind], axis2(c, STEP[s]))

    def first_end(sl):
        for c in PAIR:
            for s in PAIR:
                r1_copy(sl, 1, c, s).wait_recv()
                r1_copy(sl, 2, c, s).wait_recv()
        for c in PAIR:
            for half in PAIR:
                rows = pl.ds(rows1(sl, 3, c, half), br)
                dh[rows, :] = dh[rows, :] + r1[sl, c, half, 2] + r1[sl, c, 1 - half, 1]
        send([_Copy(r2_copy, sl, kind, c, s) for kind in (0, 1) for c in PAIR for s in PAIR])

    def second_relay(sl):
        for c in PAIR:
            for s in PAIR:
                r2_copy(sl, 0, c, s).wait_recv()
                rows = pl.ds(rows2(sl, 2, c, s), b2)
                dh[rows, :] = dh[rows, :] + r2[sl, c, s, 0]
                send([_Copy(r2_copy, sl, 2, c, s)])

    out_copies = []

    def ag2_copy(sl, c, s):
        at = pl.ds(own_rows[2 * sl + c], 2 * b2)
        return remote(dh.at[at, :], gr_out.at[at, :], ag2_s.at[sl, c, s, 0], ag2_r.at[sl, c, s, 0], axis2(c, STEP[s]))

    def own_copy(sl, c):
        at = pl.ds(own_rows[2 * sl + c], 2 * b2)
        return pltpu.make_async_copy(dh.at[at, :], gr_out.at[at, :], out_sem.at[2 * sl + c])

    def second_end(sl):
        for c in PAIR:
            for s in PAIR:
                r2_copy(sl, 1, c, s).wait_recv()
                r2_copy(sl, 2, c, s).wait_recv()
        w = w_ref[...]
        gw = jnp.zeros((1, d), F32)
        copies = []
        for c in PAIR:
            for half in PAIR:
                rows = pl.ds(rows2(sl, 3, c, half), b2)
                grad_h = dh[rows, :] + r2[sl, c, half, 2] + r2[sl, c, 1 - half, 1]
                part = pl.ds(half * b2, b2)
                resid = rown[sl, c, part, :] + hown[sl, c, part, :].astype(F32)
                inv = lax.rsqrt(jnp.mean(resid * resid, axis=-1, keepdims=True) + NORM_EPS)
                normed = resid * inv
                dn = grad_h * w
                dh[rows, :] = inv * (dn - normed * jnp.mean(dn * normed, axis=-1, keepdims=True))
                gw = gw + jnp.sum(grad_h * normed, axis=0, keepdims=True)
            copies += send([_Copy(ag2_copy, sl, c, s) for s in PAIR])
            out_copies.append(_Copy(own_copy, sl, c))
            out_copies[-1].start()
        return gw, copies

    def own_chunk(sl, c, k):
        return pl.multiple_of(sl * sl_rows + c * (sl_rows // 2) + lax.rem(place1(c) + k, 4) * (2 * br), 2 * br)

    def fwd2_copy(sl, c, s):
        rows = pl.multiple_of(own_chunk(sl, c, 0) + lax.rem(place2(c) + STEP[1 - s], 4) * (2 * b2) + s * b2, b2)
        part = gr_out.at[pl.ds(rows, b2), :]
        return remote(part, part, ag2_s.at[sl, c, s, 1], ag2_r.at[sl, c, s, 1], axis2(c, STEP[s]))

    def gather2(sl, copies):
        out = []
        for c in PAIR:
            for s in PAIR:
                copies[2 * c + s].wait_recv()
                out += send([_Copy(fwd2_copy, sl, c, s)])
        return out

    def ag1_copy(sl, c, s):
        part = gr_out.at[pl.ds(own_chunk(sl, c, 0), 2 * br), :]
        return remote(part, part, ag1_s.at[sl, c, s, 0], ag1_r.at[sl, c, s, 0], axis1(c, STEP[s]))

    def gather1_start(sl, copies):
        out = []
        for c in PAIR:
            recv(copies[2 * c:2 * c + 2])
            out_copies[2 * sl + c].make().wait()
            out += send([_Copy(ag1_copy, sl, c, s) for s in PAIR])
        return out

    def fwd1_copy(sl, c, s):
        part = gr_out.at[pl.ds(pl.multiple_of(own_chunk(sl, c, STEP[1 - s]) + s * br, br), br), :]
        return remote(part, part, ag1_s.at[sl, c, s, 1], ag1_r.at[sl, c, s, 1], axis1(c, STEP[s]))

    def gather1(sl, copies):
        out = []
        for c in PAIR:
            for s in PAIR:
                copies[2 * c + s].wait_recv()
                out += send([_Copy(fwd1_copy, sl, c, s)])
        return out

    order = (2, 1, 3, 0)
    mine = pl.ds(pl.multiple_of(core * dx, LANES), dx)
    other = pl.ds(pl.multiple_of((1 - core) * dx, LANES), dx)

    def x_index(j):
        return lax.rem(x + order[j], 4)

    def x_base(j):
        return x_index(j) * (cx - ox)

    def c_copy(j):
        rows = pl.ds(pl.multiple_of(x_base(j), 8), cx)
        return remote(ge.at[j, rows, other], crecv.at[j], c_s.at[j], c_r.at[j], partner)

    def core_end(j):
        c_copy(j).wait_recv()

        def add(i, carry):
            rows = pl.ds(pl.multiple_of(x_base(j) + i * (cx // 4), 8), cx // 4)
            ge[j, rows, mine] = ge[j, rows, mine] + crecv[j, pl.ds(pl.multiple_of(i * (cx // 4), 8), cx // 4), :]
            return carry

        lax.fori_loop(0, 4, add, 0)

    def rows_x(kind, s):
        j = 0 if kind == 0 else 3 if kind == 3 else 1 + s
        half = 1 - s if kind == 1 else s
        return j, pl.ds(pl.multiple_of(x_base(j) + half * bx, 8), bx)

    def rx_copy(kind, s):
        j, rows = rows_x(kind, s)
        return remote(ge.at[j, rows, mine], rx.at[s, kind], rx_s.at[s, kind], rx_r.at[s, kind], at_x(STEP[s]))

    def embed_stage(gbuf, hbuf):
        kb = n_tok // 4

        def loads(t):
            slot, rows = lax.rem(t, 2), pl.ds(pl.multiple_of(lax.rem(t, 4) * kb, kb), kb)
            first = lax.rem(x + jnp.where(t < 4, 2, jnp.where(t < 8, 1, jnp.where(t < 12, 3, 0))), 4)
            cols = pl.ds(pl.multiple_of(first * ox, LANES), wx)
            return (pltpu.make_async_copy(g_hbm.at[rows, cols], gbuf.at[slot], gin_sem.at[slot]),
                    pltpu.make_async_copy(h_hbm.at[rows, :], hbuf.at[slot], hin_sem.at[slot]))

        def chunk(j):
            def one(k, carry):
                t = 4 * j + k
                slot = lax.rem(t, 2)
                wait(loads(t))
                ge[j] = ge[j] + _dot(gbuf[slot], hbuf[slot], 0, 0)

                @pl.when(t + 2 < 16)
                def _():
                    start(loads(t + 2))

                return carry

            ge[j] = jnp.zeros((wx, d), F32)
            lax.fori_loop(0, 4, one, 0)
            send([_Copy(c_copy, j)])

        start(loads(0))
        start(loads(1))
        first_end(0)
        chunk(0)
        second_relay(0)
        chunk(1)
        core_end(0)
        send([_Copy(rx_copy, 0, s) for s in PAIR])
        wait(own_copies)
        gw, back = second_end(0)
        chunk(2)
        core_end(1)
        send([_Copy(rx_copy, 1, 0)])
        back = gather2(0, back)
        chunk(3)
        core_end(2)
        send([_Copy(rx_copy, 1, 1)])
        core_end(3)
        backs.append(back)
        return gw

    half_tile = pltpu.VMEM((len(chunks), rb, LANES), F32)
    tile = pltpu.VMEM((rb, LANES), F32)
    pl.run_scoped(
        logits_stage, pltpu.VMEM((2, rb, v_pad), F32), pltpu.VMEM((2, rb, mw), F32),
        pltpu.VMEM((2, rb, d), F32), pltpu.VMEM((2, rb, d), BF16), pltpu.VMEM((2, rb, d), BF16),
        half_tile, half_tile, tile)
    pl.run_scoped(
        gradient_stage, pltpu.VMEM((2, rb, v_pad), F32), pltpu.VMEM((2, rb, mw), F32),
        pltpu.VMEM((rb, v_pad), BF16), pltpu.VMEM((rb, v_pad), BF16),
        half_tile)
    backs = []
    gw0 = pl.run_scoped(embed_stage, pltpu.VMEM((2, n_tok // 4, wx), BF16), pltpu.VMEM((2, n_tok // 4, d), BF16))

    for s in PAIR:
        rx_copy(0, s).wait_recv()
        j, rows = rows_x(2, s)
        ge[j, rows, mine] = ge[j, rows, mine] + rx[s, 0]
        send([_Copy(rx_copy, 2, s)])
    back0 = gather1_start(0, backs[0])
    first_end(1)
    second_relay(1)
    last0 = gather1(0, back0)
    gw1, back1 = second_end(1)

    row8 = lax.broadcasted_iota(jnp.int32, (8, d), 0)
    small = jnp.where(row8 == 0, gw0 + gw1, jnp.where(row8 == 1, losses[0, 0:1, 0:1] + losses[1, 0:1, 0:1], 0.0))

    def small_start(phase, value):
        place = (y, z, x, core)[phase]
        smb[phase] = value
        smr[phase, place] = value
        devices = ([at_tp(k, 0) for k in OTHERS], [at_tp(0, k) for k in OTHERS], [at_x(k) for k in OTHERS], [partner])[phase]
        return send([_Copy(remote, smb.at[phase], smr.at[phase, place], sm_s.at[phase, k], sm_r.at[phase, k], device)
                     for k, device in enumerate(devices)])

    def small_end(phase, copies):
        recv(copies)
        return functools.reduce(jnp.add, [smr[phase, k] for k in range(2 if phase == 3 else 4)])

    small_step = small_start(0, small)

    def out_rows(k, first=0, size=cx):
        return pl.ds(pl.multiple_of(lax.rem(x + k, 4) * cx + first, 8), size)

    for s in PAIR:
        rx_copy(1, s).wait_recv()
        rx_copy(2, s).wait_recv()
    for half in PAIR:
        j, rows = rows_x(3, half)
        ge[j, rows, mine] = ge[j, rows, mine] + rx[half, 2] + rx[1 - half, 1]
    src = ge.at[3, pl.ds(pl.multiple_of(x_base(3), 8), cx), mine]
    dst = ge_out.at[out_rows(0), mine]
    agx = send([_Copy(remote, src, dst, agx_s.at[s, 0], agx_r.at[s, 0], at_x(STEP[s])) for s in PAIR])
    agc = send([_Copy(remote, src, dst, agc_s.at[0], agc_r.at[0], partner)])
    ge_own = pltpu.make_async_copy(src, dst, out_sem.at[4])
    ge_own.start()
    back1 = gather2(1, back1)
    small_step = small_start(1, small_end(0, small_step))
    back1 = gather1_start(1, back1)
    small_step = small_start(2, small_end(1, small_step))
    fwdx = []
    for s in PAIR:
        agx[s].wait_recv()
        part = ge_out.at[out_rows(STEP[1 - s], s * bx, bx), mine]
        fwdx += send([_Copy(remote, part, part, agx_s.at[s, 1], agx_r.at[s, 1], at_x(STEP[s]))])
        part = ge_out.at[out_rows(STEP[1 - s]), mine]
        agc += send([_Copy(remote, part, part, agc_s.at[1 + s], agc_r.at[1 + s], partner)])
    small_step = small_start(3, small_end(2, small_step))
    small_out[...] = small_end(3, small_step)
    last1 = gather1(1, back1)
    for s in PAIR:
        fwdx[s].wait_recv()
        part = ge_out.at[out_rows(2, s * bx, bx), mine]
        agc += send([_Copy(remote, part, part, agc_s.at[3 + s], agc_r.at[3 + s], partner)])
    recv(last0 + last1)

    for cp in agc:
        cp.wait_recv()
    ge_own.wait()

    def r1_sent(i, carry):
        r1_copy(lax.div(i, 12), lax.rem(lax.div(i, 4), 3), lax.rem(lax.div(i, 2), 2), lax.rem(i, 2)).wait_send()
        return carry

    lax.fori_loop(0, 24, r1_sent, 0)
    for cp in sent:
        cp.wait_send()


def solution(mesh, chunks=(1536, 1664)):
    def program(hidden, residual, targets, embedding, norm_w):
        inv_n = 1.0 / (hidden.shape[0] * hidden.shape[1])
        n_tp = mesh.shape['tp']

        def local_part(hid_loc, res_loc, tgt_loc, emb_loc, norm_vec):
            n_batch, n_seq, d = hid_loc.shape
            n_tok = n_batch * n_seq
            vocab = emb_loc.shape[0]
            v_pad = sum(chunks)
            br = n_tok // 32
            b2 = br // 4
            cx = v_pad // 4
            wx = (cx // LANES + 1) * LANES
            tiles = n_tok // (2 * LANES)
            dma = pltpu.SemaphoreType.DMA
            cube, kinds = (TWO, TWO, TWO), 3
            any_spec = pl.BlockSpec(memory_space=pl.ANY)
            vmem_spec = pl.BlockSpec(memory_space=pltpu.VMEM)
            shape = jax.ShapeDtypeStruct
            gr, ge, small, *_ = pl.pallas_call(
                functools.partial(_kernel, chunks, vocab, inv_n, n_tp),
                grid=(1,),
                in_specs=[vmem_spec, vmem_spec, pl.BlockSpec((16, d), lambda i: (vocab // 16, 0)), any_spec, any_spec, any_spec],
                out_specs=[any_spec, any_spec, vmem_spec, any_spec, any_spec, any_spec, any_spec],
                out_shape=[
                    shape((n_tok, d), F32), shape((v_pad, d), F32), shape((8, d), F32),
                    shape((n_tok, d), BF16), shape((n_tok, v_pad), F32), shape((n_tok, (len(chunks) + 1) * LANES), F32), shape((n_tok, v_pad), BF16),
                ],
                scratch_shapes=[
                    pltpu.VMEM((v_pad, d), BF16),
                    pltpu.VMEM((n_tok, d), F32),
                    pltpu.VMEM((RING, wx, d), F32),
                    pltpu.VMEM(cube + (kinds, br, d), F32),
                    pltpu.VMEM(cube + (kinds, b2, d), F32),
                    pltpu.VMEM((RING, cx, d // TWO), F32),
                    pltpu.VMEM((TWO, kinds, cx // TWO, d // TWO), F32),
                    pltpu.VMEM((TWO, kinds, tiles, LANES), F32),
                    pltpu.VMEM((TWO, RING, kinds, tiles, LANES), F32),
                    pltpu.VMEM((TWO, RING, kinds, tiles, LANES), F32),
                    pltpu.VMEM((TWO, kinds, tiles, LANES), F32),
                    pltpu.VMEM((TWO, TWO * tiles, LANES), F32),
                    pltpu.VMEM((TWO, TWO, TWO * b2, d), F32),
                    pltpu.VMEM((TWO, TWO, TWO * b2, d), BF16),
                    pltpu.VMEM((TWO, 8, LANES), F32),
                    pltpu.VMEM((RING, 8, d), F32),
                    pltpu.VMEM((RING, RING, 8, d), F32),
                    dma, dma(cube), dma(cube), dma(cube), dma(cube), dma((TWO,)), dma((TWO,)), dma(cube),
                ] + [dma((TWO, RING))] * RING + [dma(cube + (kinds,))] * RING + [dma(cube + (TWO,))] * RING + [
                    dma((5,)), dma((RING,)), dma((RING,)), dma((TWO, kinds)), dma((TWO, kinds)), dma((TWO, TWO)), dma((TWO, TWO)),
                    dma((5,)), dma((5,)), dma((RING, kinds)), dma((RING, kinds)),
                ],
                compiler_params=pltpu.CompilerParams(collective_id=0, has_side_effects=True, vmem_limit_bytes=VMEM_BYTES),
                cost_estimate=pl.CostEstimate(flops=6 * n_tok * v_pad * d, bytes_accessed=8 * n_tok * v_pad, transcendentals=0),
            )(tgt_loc.reshape(n_tok // LANES, LANES), norm_vec.reshape(1, d), emb_loc, emb_loc, res_loc.reshape(n_tok, d), hid_loc.reshape(n_tok, d))
            return small[1, 0], gr.reshape(n_batch, n_seq, d), ge[:vocab], small[0]

        sharded = jax.shard_map(
            local_part, mesh=mesh,
            in_specs=(P('dp', None, None), P('dp', None, None), P('dp', None), P('tp', None), P(None)),
            out_specs=(P(), P('dp', None, None), P('tp', None), P(None)),
            check_vma=False)
        return sharded(hidden, residual, targets, embedding, norm_w)

    return program
```

```python
import functools

import jax
import jax.numpy as jnp
from jax import lax
from jax.experimental import pallas as pl
from jax.experimental.pallas import tpu as pltpu
from jax.sharding import PartitionSpec as P

NORM_EPS = 1e-5
LANES = 128
MESH = pl.DeviceIdType.MESH
ROWS = 16
WIDE = 512
PAIR = (0, 1)
OTHERS = (1, 2, 3)
TWO = 2
RING = 4
F32 = jnp.float32
BF16 = jnp.bfloat16
VMEM_BYTES = 67_043_328
STEP = (1, 3)


class _Copy:
    def __init__(self, make, *args):
        self.make = functools.partial(make, *args)

    def start(self):
        self.make().start()

    def wait_recv(self):
        self.make().wait_recv()

    def wait_send(self):
        self.make().wait_send()


def _dot(a, b, ca, cb):
    return lax.dot_general(a, b, (((ca,), (cb,)), ((), ())), preferred_element_type=F32)


def _kernel(chunks, vocab, inv_n, n_tp,
            tgt_ref, w_ref, tail_ref, emb_hbm, res_hbm, hid_hbm,
            gr_out, ge_out, small_out, h_hbm, e_hbm, mc_hbm, g_hbm,
            emb, dh, ge, r1, r2, crecv, rx, st, sy, sz, st2, fin, rown, hown, losses, gws, smb, smr,
            emb_sem, in_sem, l_sem, e_sem, gw_sem, gin_sem, hin_sem, own_sem, sy_s, sy_r, sz_s, sz_r, r1_s, r1_r, r2_s, r2_r,
            ag2_s, ag2_r, ag1_s, ag1_r, out_sem, c_s, c_r, rx_s, rx_r, agx_s, agx_r, agc_s, agc_r, sm_s, sm_r):
    n_tok, d = dh.shape
    v_pad = emb.shape[0]
    mw = (len(chunks) + 1) * LANES
    rb = 2 * LANES
    n_blk = n_tok // rb
    br = n_tok // 32
    b2 = br // 4
    ck, sb = 2 * br, 2 * b2
    dx = d // 2
    cx = v_pad // 4
    bx = cx // 2
    wx = ge.shape[1]
    ox = (cx // LANES) * LANES
    sl_rows = n_tok // 2

    tp = lax.axis_index('tp')
    dp = lax.axis_index('dp')
    y, z = lax.rem(tp, 4), lax.div(tp, 4)
    core, x = lax.rem(dp, 2), lax.div(dp, 2)

    def at_tp(dy, dz):
        return {'tp': lax.rem(z + dz, 4) * 4 + lax.rem(y + dy, 4)}

    def at_x(k):
        return {'dp': lax.rem(x + k, 4) * 2 + core}

    partner = {'dp': x * 2 + (1 - core)}

    def axis1(c, step):
        return at_tp(step * (1 - c), step * c)

    def axis2(c, step):
        return at_tp(step * c, step * (1 - c))

    def place1(c):
        return y * (1 - c) + z * c

    def place2(c):
        return z * (1 - c) + y * c

    def remote(src, dst, send, recv, device):
        return pltpu.make_async_remote_copy(src_ref=src, dst_ref=dst, send_sem=send, recv_sem=recv,
                                            device_id=device, device_id_type=MESH)

    def start(copies):
        for cp in copies:
            cp.start()

    def wait(copies):
        for cp in copies:
            cp.wait()

    sent = []

    def send(copies):
        start(copies)
        sent.extend(copies)
        return copies

    def recv(copies):
        for cp in copies:
            cp.wait_recv()

    barrier = pltpu.get_barrier_semaphore()
    for k in OTHERS:
        for device in (at_tp(k, 0), at_tp(0, k), at_x(k)):
            pl.semaphore_signal(barrier, inc=1, device_id=device, device_id_type=MESH)
    pl.semaphore_signal(barrier, inc=1, device_id=partner, device_id_type=MESH)

    whole = (vocab // 16) * 16
    tail = jnp.where(lax.broadcasted_iota(jnp.int32, (16, d), 0) < vocab - whole, tail_ref[...].astype(F32), 0.0)
    emb[whole:whole + 16, :] = tail.astype(BF16)
    emb[whole + 16:, :] = jnp.zeros((v_pad - whole - 16, d), BF16)
    emb_copy = pltpu.make_async_copy(emb_hbm.at[pl.ds(0, whole), :], emb.at[pl.ds(0, whole), :], emb_sem)
    emb_copy.start()
    own_rows, own_copies = [], []
    for sl in PAIR:
        for c in PAIR:
            rows = pl.multiple_of(sl * sl_rows + c * (sl_rows // 2) + place1(c) * ck + place2(c) * sb, sb)
            own_rows.append(rows)
            own_copies.append(pltpu.make_async_copy(res_hbm.at[pl.ds(rows, sb), :], rown.at[sl, c], own_sem.at[sl, c, 0]))
            own_copies.append(pltpu.make_async_copy(hid_hbm.at[pl.ds(rows, sb), :], hown.at[sl, c], own_sem.at[sl, c, 1]))

    def combine(parts):
        top = functools.reduce(jnp.maximum, [p[0] for p in parts])
        total = functools.reduce(jnp.add, [p[1] * jnp.exp(p[0] - top) for p in parts])
        return top, total, functools.reduce(jnp.add, [p[2] for p in parts])

    def stats_y(sl):
        return send([_Copy(lambda k: remote(st.at[sl], sy.at[sl, k], sy_s.at[sl, k], sy_r.at[sl, k], at_tp(k, 0)), k) for k in OTHERS])

    def stats_z(sl, copies):
        recv(copies)
        parts = combine([tuple(st[sl, k] for k in range(3))] + [tuple(sy[sl, j, k] for k in range(3)) for j in OTHERS])
        for k in range(3):
            st2[sl, k] = parts[k]
        return send([_Copy(lambda k: remote(st2.at[sl], sz.at[sl, k], sz_s.at[sl, k], sz_r.at[sl, k], at_tp(0, k)), k) for k in OTHERS])

    tiles_sl = sl_rows // LANES

    def stats_end(sl, copies):
        recv(copies)
        top, total, picked = combine([tuple(st2[sl, k] for k in range(3))] + [tuple(sz[sl, j, k] for k in range(3)) for j in OTHERS])
        fin[0, sl * tiles_sl:(sl + 1) * tiles_sl, :] = top
        fin[1, sl * tiles_sl:(sl + 1) * tiles_sl, :] = inv_n / total
        part = (top + jnp.log(total) - picked) * (inv_n / n_tp)
        losses[sl] = jnp.sum(jnp.sum(part, axis=0, keepdims=True), axis=1, keepdims=True) + jnp.zeros((8, LANES), F32)

    ahead = {}

    def block_rows(i):
        return pl.ds(pl.multiple_of(i * rb, rb), rb)

    def logits_stage(ebuf, mcbuf, rbuf, hbuf, hobuf, sums, picks, ids):
        def kept(v, first, size, k, width):
            return v, pl.ds((k // d) * rb + first, size), pl.ds(k % d, width)

        def loads(i):
            slot, rows = lax.rem(i, 2), block_rows(i)
            return (pltpu.make_async_copy(res_hbm.at[rows, :], rbuf.at[slot], in_sem.at[slot, 0, 0]),
                    pltpu.make_async_copy(hid_hbm.at[rows, :], hbuf.at[slot], in_sem.at[slot, 0, 1]))

        def stores(i):
            slot, rows = lax.rem(i, 2), block_rows(i)
            return (pltpu.make_async_copy(hobuf.at[slot], h_hbm.at[rows, :], l_sem.at[slot, 0, 0]),
                    pltpu.make_async_copy(ebuf.at[slot], e_hbm.at[rows, :], l_sem.at[slot, 0, 1]),
                    pltpu.make_async_copy(mcbuf.at[slot], mc_hbm.at[rows, :], l_sem.at[slot, 1, 0]))

        step = {}

        def one(i, carry):
            slot = lax.rem(i, 2)

            @pl.when(i == n_blk // 2)
            def _():
                pl.semaphore_wait(barrier, 10)
                step['y'] = stats_y(0)
                start(own_copies)

            @pl.when(i == 3 * n_blk // 4)
            def _():
                step['z'] = stats_z(0, step['y'])

            wait(loads(i))

            @pl.when(i >= 2)
            def _():
                wait(stores(i - 2))

            resid = rbuf[slot] + hbuf[slot].astype(F32)
            inv = lax.rsqrt(jnp.mean(resid * resid, axis=-1, keepdims=True) + NORM_EPS)
            h = (resid * inv * w_ref[...]).astype(BF16)
            hobuf[slot] = h
            for j in range(rb // LANES):
                row = (tgt_ref[pl.ds(i * (rb // LANES) + j, 1), :] - tp * vocab).astype(F32)
                col = jnp.broadcast_to(row, (LANES, LANES)).T
                ids[j * LANES:(j + 1) * LANES, :] = jnp.where((col >= 0) & (col < vocab), col, -1.0)
            mcbuf[slot, :, len(chunks) * LANES:] = ids[...]

            def finish(v):
                at = sum(chunks[:v])

                def some(r, carry):
                    first = pl.multiple_of(r * ROWS, ROWS)
                    rows = pl.ds(first, ROWS)
                    tgt = ids[rows, :].astype(jnp.int32)
                    tiles = [ge[kept(v, first, ROWS, k, LANES)] for k in range(0, chunks[v], LANES)]
                    pick = jnp.zeros((ROWS, LANES), F32)
                    for k, tile in enumerate(tiles):
                        pick = pick + jnp.where(lane == tgt - (at + k * LANES), tile, 0.0)
                    real = lane < vocab - (at + chunks[v] - LANES)
                    if at + chunks[v] > vocab:
                        top = functools.reduce(jnp.maximum, tiles[:-1] + [jnp.where(real, tiles[-1], -jnp.inf)])
                    else:
                        top = functools.reduce(jnp.maximum, tiles)
                    total = jnp.zeros((ROWS, LANES), F32)
                    for k, tile in enumerate(tiles):
                        e = jnp.exp(tile - top)
                        if at + (k + 1) * LANES > vocab:
                            e = jnp.where(real, e, 0.0)
                        ebuf[slot, rows, at + k * LANES:at + (k + 1) * LANES] = e
                        total = total + e
                    mcbuf[slot, rows, v * LANES:(v + 1) * LANES] = top
                    sums[v, rows, :] = total
                    picks[v, rows, :] = pick
                    return carry

                lax.fori_loop(0, rb // ROWS, some, 0, unroll=True)

            lane = lax.broadcasted_iota(jnp.int32, (ROWS, LANES), 1)
            at = 0
            for v, width in enumerate(chunks):
                for k in range(0, width, d):
                    part = min(d, width - k)
                    ge[kept(v, 0, rb, k, part)] = _dot(h, emb[at + k:at + k + part, :], 1, 1)
                if v:
                    finish(v - 1)
                at += width
            finish(len(chunks) - 1)
            maxes = [mcbuf[slot, :, v * LANES:(v + 1) * LANES] for v in range(len(chunks))]
            top = jnp.max(functools.reduce(jnp.maximum, maxes), axis=-1, keepdims=True)
            total = functools.reduce(jnp.add, [sums[v] * jnp.exp(m - top) for v, m in enumerate(maxes)])
            total = jnp.sum(total, axis=-1, keepdims=True)
            picked = jnp.sum(functools.reduce(jnp.add, [picks[v] for v in range(len(chunks))]), axis=-1, keepdims=True)
            lane = lax.broadcasted_iota(jnp.int32, (rb, LANES), 1)
            table = jnp.where(lane == 0, top, jnp.where(lane == 1, total, picked))
            sl = lax.div(i, n_blk // 2)
            for j in range(rb // LANES):
                tile = table[j * LANES:(j + 1) * LANES, :].T
                row = pl.ds((i - sl * (n_blk // 2)) * (rb // LANES) + j, 1)
                for k in range(3):
                    st[sl, k, row, :] = tile[k:k + 1, :]
            start(stores(i))

            @pl.when(i + 2 < n_blk)
            def _():
                start(loads(i + 2))

            return carry

        start(loads(0))
        start(loads(1))
        emb_copy.wait()
        lax.fori_loop(0, n_blk, one, 0)
        ahead['y'] = stats_y(1)
        wait(stores(n_blk - 2))
        wait(stores(n_blk - 1))
        stats_end(0, step['z'])

    def rows1(sl, kind, c, s):
        step = 1 + 2 * s
        chunk = lax.rem(place1(c) + jnp.where(kind == 0, 2, jnp.where(kind == 3, 0, step)), 4)
        half = jnp.where(kind == 1, 1 - s, s)
        return pl.multiple_of(sl * sl_rows + c * (sl_rows // 2) + chunk * ck + half * br, br)

    def r1_copy(sl, kind, c, s):
        rows = pl.ds(rows1(sl, kind, c, s), br)
        return remote(dh.at[rows, :], r1.at[sl, c, s, kind], r1_s.at[sl, c, s, kind], r1_r.at[sl, c, s, kind], axis1(c, 1 + 2 * s))

    def gradient_stage(ebuf, mcbuf, gbuf0, gbuf1, spread):
        gbufs = (gbuf0, gbuf1)
        row_id = lax.broadcasted_iota(jnp.int32, (LANES, LANES), 0)
        lane = lax.broadcasted_iota(jnp.int32, (ROWS, WIDE), 1)

        def piece(b, c, s):
            b = lax.rem(b, n_blk)
            return rows1(lax.div(b, 8), lax.rem(lax.div(b, 2), 4), c, s)

        def loads(b, c):
            out = []
            for s in PAIR:
                rows = pl.ds(piece(b, c, s), br)
                part = pl.ds(s * br, br)
                out.append(pltpu.make_async_copy(e_hbm.at[rows, :], ebuf.at[c, part, :], e_sem.at[c, s, 0]))
                out.append(pltpu.make_async_copy(mc_hbm.at[rows, :], mcbuf.at[c, part, :], e_sem.at[c, s, 1]))
            return out

        def stores(b, c):
            return [pltpu.make_async_copy(gbufs[c].at[pl.ds(s * br, br), :], g_hbm.at[pl.ds(piece(b, c, s), br), :], gw_sem.at[c, s, 0])
                    for s in PAIR]

        def prepare(b, c):
            for s in PAIR:
                at = lax.div(piece(b, c, s), LANES)
                cols = jnp.where(row_id == 0, fin[0, pl.ds(at, 1), :], fin[1, pl.ds(at, 1), :]).T
                part = slice(s * br, (s + 1) * br)
                for v in range(len(chunks)):
                    lanes = slice(v * LANES, (v + 1) * LANES)
                    spread[v, part, :] = jnp.exp(mcbuf[c, part, lanes] - cols[:, 0:1]) * cols[:, 1:2]

        def make_g(c, unroll=True):
            def some(r, carry):
                rows = pl.ds(pl.multiple_of(r * ROWS, ROWS), ROWS)
                tgt = mcbuf[c, rows, len(chunks) * LANES:].astype(jnp.int32)
                at = 0
                for v, width in enumerate(chunks):
                    scale = spread[v, rows, :]
                    for k in range(at, at + width, WIDE):
                        n = min(WIDE, at + width - k)
                        hit = lane[:, :n] == jnp.concatenate([tgt - k] * (n // LANES), axis=1)
                        g = ebuf[c, rows, k:k + n] * jnp.concatenate([scale] * (n // LANES), axis=1) - jnp.where(hit, inv_n, 0.0)
                        gbufs[c][rows, k:k + n] = g.astype(BF16)
                    at += width
                return carry

            lax.fori_loop(0, rb // ROWS, some, 0, unroll=unroll)

        def step(b, c):
            nb, nc = b + 1, 1 - c
            sl, kind = lax.div(b, 8), lax.rem(lax.div(b, 2), 4)
            wait(loads(nb, nc))

            @pl.when(nb >= 2)
            def _():
                wait(stores(nb - 2, nc))

            prepare(nb, nc)
            rows = [pl.ds(rows1(sl, kind, c, s), br) for s in PAIR]

            make_g(nc)
            value = _dot(gbufs[c][...], emb[...], 1, 0)
            for s in PAIR:
                dh[rows[s], :] = value[s * br:(s + 1) * br, :]

            @pl.when(nb < n_blk)
            def _():
                start(stores(nb, nc))

            @pl.when(nb + 2 <= n_blk)
            def _():
                start(loads(nb + 2, nc))

            @pl.when(kind < 2)
            def _():
                for s in PAIR:
                    r1_copy(sl, kind, c, s).start()

            @pl.when(kind == 2)
            def _():
                for s in PAIR:
                    r1_copy(sl, 0, c, s).wait_recv()
                    rows = pl.ds(rows1(sl, kind, c, s), br)
                    dh[rows, :] = dh[rows, :] + r1[sl, c, s, 0]
                    r1_copy(sl, 2, c, s).start()

        def pair(kk, carry):
            @pl.when(kk == 2)
            def _():
                stats_end(1, ahead['z'])

            @pl.when(kk == 6)
            def _():
                first_end(0)

            step(2 * kk, 0)
            step(2 * kk + 1, 1)
            return carry

        start(loads(0, 0))
        start(loads(1, 1))
        wait(loads(0, 0))
        prepare(0, 0)
        make_g(0, False)
        start(stores(0, 0))
        start(loads(2, 0))
        ahead['z'] = stats_z(1, ahead['y'])
        lax.fori_loop(0, n_blk // 2, pair, 0)
        wait(stores(n_blk - 1, 1))

    def rows2(sl, kind, c, s):
        chunk = lax.rem(place2(c) + (2 if kind == 0 else 0 if kind == 3 else STEP[s]), 4)
        half = 1 - s if kind == 1 else s
        return pl.multiple_of(sl * sl_rows + c * (sl_rows // 2) + place1(c) * ck + chunk * sb + half * b2, b2)

    def r2_copy(sl, kind, c, s):
        rows = pl.ds(rows2(sl, kind, c, s), b2)
        return remote(dh.at[rows, :], r2.at[sl, c, s, kind], r2_s.at[sl, c, s, kind], r2_r.at[sl, c, s, kind], axis2(c, STEP[s]))

    def first_end(sl):
        for c in PAIR:
            for s in PAIR:
                r1_copy(sl, 1, c, s).wait_recv()
                r1_copy(sl, 2, c, s).wait_recv()
        for c in PAIR:
            for half in PAIR:
                rows = pl.ds(rows1(sl, 3, c, half), br)
                dh[rows, :] = dh[rows, :] + r1[sl, c, half, 2] + r1[sl, c, 1 - half, 1]
        send([_Copy(r2_copy, sl, kind, c, s) for kind in (0, 1) for c in PAIR for s in PAIR])

    def second_relay(sl):
        for c in PAIR:
            for s in PAIR:
                r2_copy(sl, 0, c, s).wait_recv()
                rows = pl.ds(rows2(sl, 2, c, s), b2)
                dh[rows, :] = dh[rows, :] + r2[sl, c, s, 0]
                send([_Copy(r2_copy, sl, 2, c, s)])

    out_copies = []
    held = {}

    def ag2_copy(sl, c, s):
        at = pl.ds(own_rows[2 * sl + c], sb)
        return remote(dh.at[at, :], gr_out.at[at, :], ag2_s.at[sl, c, s, 0], ag2_r.at[sl, c, s, 0], axis2(c, STEP[s]))

    def own_copy(sl, c):
        at = pl.ds(own_rows[2 * sl + c], sb)
        return pltpu.make_async_copy(dh.at[at, :], gr_out.at[at, :], out_sem.at[2 * sl + c])

    def second_end(sl):
        for c in PAIR:
            for s in PAIR:
                r2_copy(sl, 1, c, s).wait_recv()
                r2_copy(sl, 2, c, s).wait_recv()
        w = w_ref[...]
        gw = jnp.zeros((1, d), F32)
        copies = []
        for c in PAIR:
            for half in PAIR:
                rows = pl.ds(rows2(sl, 3, c, half), b2)
                grad_h = dh[rows, :] + r2[sl, c, half, 2] + r2[sl, c, 1 - half, 1]
                part = pl.ds(half * b2, b2)
                resid = rown[sl, c, part, :] + hown[sl, c, part, :].astype(F32)
                inv = lax.rsqrt(jnp.mean(resid * resid, axis=-1, keepdims=True) + NORM_EPS)
                normed = resid * inv
                dn = grad_h * w
                dh[rows, :] = inv * (dn - normed * jnp.mean(dn * normed, axis=-1, keepdims=True))
                gw = gw + jnp.sum(grad_h * normed, axis=0, keepdims=True)
            copies += send([_Copy(ag2_copy, sl, c, s) for s in PAIR])
            out_copies.append(_Copy(own_copy, sl, c))
            out_copies[-1].start()
        gws[sl] = jnp.broadcast_to(gw, (8, d))
        return copies

    def own_chunk(sl, c, k):
        return pl.multiple_of(sl * sl_rows + c * (sl_rows // 2) + lax.rem(place1(c) + k, 4) * ck, ck)

    def fwd2_copy(sl, c, s):
        rows = pl.multiple_of(own_chunk(sl, c, 0) + lax.rem(place2(c) + STEP[1 - s], 4) * sb + s * b2, b2)
        part = gr_out.at[pl.ds(rows, b2), :]
        return remote(part, part, ag2_s.at[sl, c, s, 1], ag2_r.at[sl, c, s, 1], axis2(c, STEP[s]))

    def gather2(sl, copies):
        out = []
        for c in PAIR:
            for s in PAIR:
                copies[2 * c + s].wait_recv()
                out += send([_Copy(fwd2_copy, sl, c, s)])
        return out

    def ag1_copy(sl, c, s):
        part = gr_out.at[pl.ds(own_chunk(sl, c, 0), ck), :]
        return remote(part, part, ag1_s.at[sl, c, s, 0], ag1_r.at[sl, c, s, 0], axis1(c, STEP[s]))

    def gather1_start(sl, copies):
        out = []
        for c in PAIR:
            recv(copies[2 * c:2 * c + 2])
            out_copies[2 * sl + c].make().wait()
            out += send([_Copy(ag1_copy, sl, c, s) for s in PAIR])
        return out

    def fwd1_copy(sl, c, s):
        part = gr_out.at[pl.ds(pl.multiple_of(own_chunk(sl, c, STEP[1 - s]) + s * br, br), br), :]
        return remote(part, part, ag1_s.at[sl, c, s, 1], ag1_r.at[sl, c, s, 1], axis1(c, STEP[s]))

    def gather1(sl, copies):
        out = []
        for c in PAIR:
            for s in PAIR:
                copies[2 * c + s].wait_recv()
                out += send([_Copy(fwd1_copy, sl, c, s)])
        return out

    order = (2, 1, 3, 0)
    mine = pl.ds(pl.multiple_of(core * dx, LANES), dx)
    other = pl.ds(pl.multiple_of((1 - core) * dx, LANES), dx)

    def x_index(j):
        return lax.rem(x + order[j], 4)

    def x_base(j):
        return x_index(j) * (cx - ox)

    def c_copy(j):
        rows = pl.ds(pl.multiple_of(x_base(j), 8), cx)
        return remote(ge.at[j, rows, other], crecv.at[j], c_s.at[j], c_r.at[j], partner)

    def core_end(j):
        c_copy(j).wait_recv()

        def add(i, carry):
            rows = pl.ds(pl.multiple_of(x_base(j) + i * (cx // 4), 8), cx // 4)
            ge[j, rows, mine] = ge[j, rows, mine] + crecv[j, pl.ds(pl.multiple_of(i * (cx // 4), 8), cx // 4), :]
            return carry

        lax.fori_loop(0, 4, add, 0)

    def rows_x(kind, s):
        j = 0 if kind == 0 else 3 if kind == 3 else 1 + s
        half = 1 - s if kind == 1 else s
        return j, pl.ds(pl.multiple_of(x_base(j) + half * bx, 8), bx)

    def rx_copy(kind, s):
        j, rows = rows_x(kind, s)
        return remote(ge.at[j, rows, mine], rx.at[s, kind], rx_s.at[s, kind], rx_r.at[s, kind], at_x(STEP[s]))

    def embed_stage(gbuf, hbuf):
        kb = n_tok // 4

        def loads(t):
            slot, rows = lax.rem(t, 2), pl.ds(pl.multiple_of(lax.rem(t, 4) * kb, kb), kb)
            first = lax.rem(x + jnp.where(t < 4, 2, jnp.where(t < 8, 1, jnp.where(t < 12, 3, 0))), 4)
            cols = pl.ds(pl.multiple_of(first * ox, LANES), wx)
            return (pltpu.make_async_copy(g_hbm.at[rows, cols], gbuf.at[slot], gin_sem.at[slot]),
                    pltpu.make_async_copy(h_hbm.at[rows, :], hbuf.at[slot], hin_sem.at[slot]))

        def chunk(j, middle):
            def one(k, carry):
                pl.when(k == 2)(middle)
                t = 4 * j + k
                slot = lax.rem(t, 2)
                wait(loads(t))
                ge[j] = ge[j] + _dot(gbuf[slot], hbuf[slot], 0, 0)

                @pl.when(t + 2 < 16)
                def _():
                    start(loads(t + 2))

                return carry

            ge[j] = jnp.zeros((wx, d), F32)
            lax.fori_loop(0, 4, one, 0)
            send([_Copy(c_copy, j)])

        def middle1():
            core_end(0)
            send([_Copy(rx_copy, 0, s) for s in PAIR])
            held[0] = second_end(0)

        def middle2():
            core_end(1)
            send([_Copy(rx_copy, 1, 0)])
            second_relay(1)
            held[0] = gather1_start(0, held[0])

        def middle3():
            core_end(2)
            send([_Copy(rx_copy, 1, 1)])
            for s in PAIR:
                rx_copy(0, s).wait_recv()
                j, rows = rows_x(2, s)
                ge[j, rows, mine] = ge[j, rows, mine] + rx[s, 0]
                send([_Copy(rx_copy, 2, s)])

        start(loads(0))
        start(loads(1))
        wait(own_copies)
        chunk(0, functools.partial(second_relay, 0))
        chunk(1, middle1)
        held[0] = gather2(0, held[0])
        first_end(1)
        chunk(2, middle2)
        held[1] = second_end(1)
        chunk(3, middle3)
        core_end(3)

    half_tile = pltpu.VMEM((len(chunks), rb, LANES), F32)
    tile = pltpu.VMEM((rb, LANES), F32)
    pl.run_scoped(
        logits_stage, pltpu.VMEM((2, rb, v_pad), F32), pltpu.VMEM((2, rb, mw), F32),
        pltpu.VMEM((2, rb, d), F32), pltpu.VMEM((2, rb, d), BF16), pltpu.VMEM((2, rb, d), BF16),
        half_tile, half_tile, tile)
    pl.run_scoped(
        gradient_stage, pltpu.VMEM((2, rb, v_pad), F32), pltpu.VMEM((2, rb, mw), F32),
        pltpu.VMEM((rb, v_pad), BF16), pltpu.VMEM((rb, v_pad), BF16),
        half_tile)
    pl.run_scoped(embed_stage, pltpu.VMEM((2, n_tok // 4, wx), BF16), pltpu.VMEM((2, n_tok // 4, d), BF16))

    row8 = lax.broadcasted_iota(jnp.int32, (8, d), 0)
    small = jnp.where(row8 == 0, gws[0] + gws[1], jnp.where(row8 == 1, losses[0, 0:1, 0:1] + losses[1, 0:1, 0:1], 0.0))

    def small_start(phase, value):
        place = (y, z, x, core)[phase]
        smb[phase] = value
        smr[phase, place] = value
        devices = ([at_tp(k, 0) for k in OTHERS], [at_tp(0, k) for k in OTHERS], [at_x(k) for k in OTHERS], [partner])[phase]
        return send([_Copy(remote, smb.at[phase], smr.at[phase, place], sm_s.at[phase, k], sm_r.at[phase, k], device)
                     for k, device in enumerate(devices)])

    def small_end(phase, copies):
        recv(copies)
        return functools.reduce(jnp.add, [smr[phase, k] for k in range(2 if phase == 3 else 4)])

    small_step = small_start(0, small)
    last0 = gather1(0, held[0])
    back1 = gather1_start(1, gather2(1, held[1]))
    small_step = small_start(1, small_end(0, small_step))

    def out_rows(k, first=0, size=cx):
        return pl.ds(pl.multiple_of(lax.rem(x + k, 4) * cx + first, 8), size)

    for s in PAIR:
        rx_copy(1, s).wait_recv()
        rx_copy(2, s).wait_recv()
    for half in PAIR:
        j, rows = rows_x(3, half)
        ge[j, rows, mine] = ge[j, rows, mine] + rx[half, 2] + rx[1 - half, 1]
    src = ge.at[3, pl.ds(pl.multiple_of(x_base(3), 8), cx), mine]
    dst = ge_out.at[out_rows(0), mine]
    agx = send([_Copy(remote, src, dst, agx_s.at[s, 0], agx_r.at[s, 0], at_x(STEP[s])) for s in PAIR])
    agc = send([_Copy(remote, src, dst, agc_s.at[0], agc_r.at[0], partner)])
    ge_own = pltpu.make_async_copy(src, dst, out_sem.at[4])
    ge_own.start()
    small_step = small_start(2, small_end(1, small_step))
    last1 = gather1(1, back1)
    fwdx = []
    for s in PAIR:
        agx[s].wait_recv()
        part = ge_out.at[out_rows(STEP[1 - s], s * bx, bx), mine]
        fwdx += send([_Copy(remote, part, part, agx_s.at[s, 1], agx_r.at[s, 1], at_x(STEP[s]))])
        part = ge_out.at[out_rows(STEP[1 - s]), mine]
        agc += send([_Copy(remote, part, part, agc_s.at[1 + s], agc_r.at[1 + s], partner)])
    small_step = small_start(3, small_end(2, small_step))
    for s in PAIR:
        fwdx[s].wait_recv()
        part = ge_out.at[out_rows(2, s * bx, bx), mine]
        agc += send([_Copy(remote, part, part, agc_s.at[3 + s], agc_r.at[3 + s], partner)])
    small_out[...] = small_end(3, small_step)
    recv(last0 + last1)

    for cp in agc:
        cp.wait_recv()
    ge_own.wait()

    def r1_sent(i, carry):
        r1_copy(lax.div(i, 12), lax.rem(lax.div(i, 4), 3), lax.rem(lax.div(i, 2), 2), lax.rem(i, 2)).wait_send()
        return carry

    lax.fori_loop(0, 24, r1_sent, 0)
    for cp in sent:
        cp.wait_send()


def solution(mesh, chunks=(1536, 1664)):
    def program(hidden, residual, targets, embedding, norm_w):
        inv_n = 1.0 / (hidden.shape[0] * hidden.shape[1])
        n_tp = mesh.shape['tp']

        def local_part(hid_loc, res_loc, tgt_loc, emb_loc, norm_vec):
            n_batch, n_seq, d = hid_loc.shape
            n_tok = n_batch * n_seq
            vocab = emb_loc.shape[0]
            v_pad = sum(chunks)
            br = n_tok // 32
            b2 = br // 4
            cx = v_pad // 4
            wx = (cx // LANES + 1) * LANES
            tiles = n_tok // (2 * LANES)
            dma = pltpu.SemaphoreType.DMA
            cube, kinds = (TWO, TWO, TWO), 3
            any_spec = pl.BlockSpec(memory_space=pl.ANY)
            vmem_spec = pl.BlockSpec(memory_space=pltpu.VMEM)
            shape = jax.ShapeDtypeStruct
            gr, ge, small, *_ = pl.pallas_call(
                functools.partial(_kernel, chunks, vocab, inv_n, n_tp),
                grid=(1,),
                in_specs=[vmem_spec, vmem_spec, pl.BlockSpec((16, d), lambda i: (vocab // 16, 0)), any_spec, any_spec, any_spec],
                out_specs=[any_spec, any_spec, vmem_spec, any_spec, any_spec, any_spec, any_spec],
                out_shape=[
                    shape((n_tok, d), F32), shape((v_pad, d), F32), shape((8, d), F32),
                    shape((n_tok, d), BF16), shape((n_tok, v_pad), F32), shape((n_tok, (len(chunks) + 1) * LANES), F32), shape((n_tok, v_pad), BF16),
                ],
                scratch_shapes=[
                    pltpu.VMEM((v_pad, d), BF16),
                    pltpu.VMEM((n_tok, d), F32),
                    pltpu.VMEM((RING, wx, d), F32),
                    pltpu.VMEM(cube + (kinds, br, d), F32),
                    pltpu.VMEM(cube + (kinds, b2, d), F32),
                    pltpu.VMEM((RING, cx, d // TWO), F32),
                    pltpu.VMEM((TWO, kinds, cx // TWO, d // TWO), F32),
                    pltpu.VMEM((TWO, kinds, tiles, LANES), F32),
                    pltpu.VMEM((TWO, RING, kinds, tiles, LANES), F32),
                    pltpu.VMEM((TWO, RING, kinds, tiles, LANES), F32),
                    pltpu.VMEM((TWO, kinds, tiles, LANES), F32),
                    pltpu.VMEM((TWO, TWO * tiles, LANES), F32),
                    pltpu.VMEM((TWO, TWO, TWO * b2, d), F32),
                    pltpu.VMEM((TWO, TWO, TWO * b2, d), BF16),
                    pltpu.VMEM((TWO, 8, LANES), F32),
                    pltpu.VMEM((TWO, 8, d), F32),
                    pltpu.VMEM((RING, 8, d), F32),
                    pltpu.VMEM((RING, RING, 8, d), F32),
                    dma, dma(cube), dma(cube), dma(cube), dma(cube), dma((TWO,)), dma((TWO,)), dma(cube),
                ] + [dma((TWO, RING))] * RING + [dma(cube + (kinds,))] * RING + [dma(cube + (TWO,))] * RING + [
                    dma((5,)), dma((RING,)), dma((RING,)), dma((TWO, kinds)), dma((TWO, kinds)), dma((TWO, TWO)), dma((TWO, TWO)),
                    dma((5,)), dma((5,)), dma((RING, kinds)), dma((RING, kinds)),
                ],
                compiler_params=pltpu.CompilerParams(collective_id=0, has_side_effects=True, vmem_limit_bytes=VMEM_BYTES),
                cost_estimate=pl.CostEstimate(flops=6 * n_tok * v_pad * d, bytes_accessed=8 * n_tok * v_pad, transcendentals=0),
            )(tgt_loc.reshape(n_tok // LANES, LANES), norm_vec.reshape(1, d), emb_loc, emb_loc, res_loc.reshape(n_tok, d), hid_loc.reshape(n_tok, d))
            return small[1, 0], gr.reshape(n_batch, n_seq, d), ge[:vocab], small[0]

        sharded = jax.shard_map(
            local_part, mesh=mesh,
            in_specs=(P('dp', None, None), P('dp', None, None), P('dp', None), P('tp', None), P(None)),
            out_specs=(P(), P('dp', None, None), P('tp', None), P(None)),
            check_vma=False)
        return sharded(hidden, residual, targets, embedding, norm_w)

    return program
```

```python
import functools

import jax
import jax.numpy as jnp
from jax import lax
from jax.experimental import pallas as pl
from jax.experimental.pallas import tpu as pltpu
from jax.sharding import PartitionSpec as P

NORM_EPS = 1e-5
LANES = 128
MESH = pl.DeviceIdType.MESH
ROWS = 16
WIDE = 512
PAIR = (0, 1)
OTHERS = (1, 2, 3)
TWO = 2
RING = 4
F32 = jnp.float32
BF16 = jnp.bfloat16
VMEM_BYTES = 67_043_328
STEP = (1, 3)


class _Copy:
    def __init__(self, make, *args):
        self.make = functools.partial(make, *args)

    def start(self):
        self.make().start()

    def wait_recv(self):
        self.make().wait_recv()

    def wait_send(self):
        self.make().wait_send()


def _dot(a, b, ca, cb):
    return lax.dot_general(a, b, (((ca,), (cb,)), ((), ())), preferred_element_type=F32)


def _kernel(chunks, vocab, inv_n, n_tp,
            tgt_ref, w_ref, tail_ref, emb_hbm, res_hbm, hid_hbm,
            gr_out, ge_out, small_out, h_hbm, e_hbm, mc_hbm, g_hbm,
            emb, dh, ge, r1, r2, crecv, rx, st, sy, sz, st2, fin, rown, hown, losses, gws, smb, smr,
            emb_sem, in_sem, l_sem, e_sem, gw_sem, gin_sem, hin_sem, own_sem, sy_s, sy_r, sz_s, sz_r, r1_s, r1_r, r2_s, r2_r,
            ag2_s, ag2_r, ag1_s, ag1_r, out_sem, c_s, c_r, rx_s, rx_r, agx_s, agx_r, agc_s, agc_r, sm_s, sm_r):
    n_tok, d = dh.shape
    v_pad = emb.shape[0]
    mw = (len(chunks) + 1) * LANES
    rb = 2 * LANES
    n_blk = n_tok // rb
    br = n_tok // 32
    b2 = br // 4
    ck, sb = 2 * br, 2 * b2
    dx = d // 2
    cx = v_pad // 4
    bx = cx // 2
    wx = ge.shape[1]
    ox = (cx // LANES) * LANES
    sl_rows = n_tok // 2

    tp = lax.axis_index('tp')
    dp = lax.axis_index('dp')
    y, z = lax.rem(tp, 4), lax.div(tp, 4)
    core, x = lax.rem(dp, 2), lax.div(dp, 2)

    def at_tp(dy, dz):
        return {'tp': lax.rem(z + dz, 4) * 4 + lax.rem(y + dy, 4)}

    def at_x(k):
        return {'dp': lax.rem(x + k, 4) * 2 + core}

    partner = {'dp': x * 2 + (1 - core)}

    def axis1(c, step):
        return at_tp(step * (1 - c), step * c)

    def axis2(c, step):
        return at_tp(step * c, step * (1 - c))

    def place1(c):
        return y * (1 - c) + z * c

    def place2(c):
        return z * (1 - c) + y * c

    def remote(src, dst, send, recv, device):
        return pltpu.make_async_remote_copy(src_ref=src, dst_ref=dst, send_sem=send, recv_sem=recv,
                                            device_id=device, device_id_type=MESH)

    def start(copies):
        for cp in copies:
            cp.start()

    def wait(copies):
        for cp in copies:
            cp.wait()

    sent = []

    def send(copies):
        start(copies)
        sent.extend(copies)
        return copies

    def recv(copies):
        for cp in copies:
            cp.wait_recv()

    barrier = pltpu.get_barrier_semaphore()
    for k in OTHERS:
        for device in (at_tp(k, 0), at_tp(0, k), at_x(k)):
            pl.semaphore_signal(barrier, inc=1, device_id=device, device_id_type=MESH)
    pl.semaphore_signal(barrier, inc=1, device_id=partner, device_id_type=MESH)

    whole = (vocab // 16) * 16
    tail = jnp.where(lax.broadcasted_iota(jnp.int32, (16, d), 0) < vocab - whole, tail_ref[...].astype(F32), 0.0)
    emb[whole:whole + 16, :] = tail.astype(BF16)
    emb[whole + 16:, :] = jnp.zeros((v_pad - whole - 16, d), BF16)
    emb_copy = pltpu.make_async_copy(emb_hbm.at[pl.ds(0, whole), :], emb.at[pl.ds(0, whole), :], emb_sem)
    emb_copy.start()
    own_rows, own_copies = [], []
    for sl in PAIR:
        for c in PAIR:
            rows = pl.multiple_of(sl * sl_rows + c * (sl_rows // 2) + place1(c) * ck + place2(c) * sb, sb)
            own_rows.append(rows)
            own_copies.append(pltpu.make_async_copy(res_hbm.at[pl.ds(rows, sb), :], rown.at[sl, c], own_sem.at[sl, c, 0]))
            own_copies.append(pltpu.make_async_copy(hid_hbm.at[pl.ds(rows, sb), :], hown.at[sl, c], own_sem.at[sl, c, 1]))

    def combine(parts):
        top = functools.reduce(jnp.maximum, [p[0] for p in parts])
        total = functools.reduce(jnp.add, [p[1] * jnp.exp(p[0] - top) for p in parts])
        return top, total, functools.reduce(jnp.add, [p[2] for p in parts])

    def stats_y(sl):
        return send([_Copy(lambda k: remote(st.at[sl], sy.at[sl, k], sy_s.at[sl, k], sy_r.at[sl, k], at_tp(k, 0)), k) for k in OTHERS])

    def stats_z(sl, copies):
        recv(copies)
        parts = combine([tuple(st[sl, k] for k in range(3))] + [tuple(sy[sl, j, k] for k in range(3)) for j in OTHERS])
        for k in range(3):
            st2[sl, k] = parts[k]
        return send([_Copy(lambda k: remote(st2.at[sl], sz.at[sl, k], sz_s.at[sl, k], sz_r.at[sl, k], at_tp(0, k)), k) for k in OTHERS])

    tiles_sl = sl_rows // LANES

    def stats_end(sl, copies):
        recv(copies)
        top, total, picked = combine([tuple(st2[sl, k] for k in range(3))] + [tuple(sz[sl, j, k] for k in range(3)) for j in OTHERS])
        fin[0, sl * tiles_sl:(sl + 1) * tiles_sl, :] = top
        fin[1, sl * tiles_sl:(sl + 1) * tiles_sl, :] = inv_n / total
        part = (top + jnp.log(total) - picked) * (inv_n / n_tp)
        losses[sl] = jnp.sum(jnp.sum(part, axis=0, keepdims=True), axis=1, keepdims=True) + jnp.zeros((8, LANES), F32)

    ahead = {}

    def block_rows(i):
        return pl.ds(pl.multiple_of(i * rb, rb), rb)

    def logits_stage(ebuf, mcbuf, rbuf, hbuf, hobuf, sums, picks, ids):
        def kept(v, first, size, k, width):
            return v, pl.ds((k // d) * rb + first, size), pl.ds(k % d, width)

        def loads(i):
            slot, rows = lax.rem(i, 2), block_rows(i)
            return (pltpu.make_async_copy(res_hbm.at[rows, :], rbuf.at[slot], in_sem.at[slot, 0, 0]),
                    pltpu.make_async_copy(hid_hbm.at[rows, :], hbuf.at[slot], in_sem.at[slot, 0, 1]))

        def stores(i):
            slot, rows = lax.rem(i, 2), block_rows(i)
            return (pltpu.make_async_copy(hobuf.at[slot], h_hbm.at[rows, :], l_sem.at[slot, 0, 0]),
                    pltpu.make_async_copy(ebuf.at[slot], e_hbm.at[rows, :], l_sem.at[slot, 0, 1]),
                    pltpu.make_async_copy(mcbuf.at[slot], mc_hbm.at[rows, :], l_sem.at[slot, 1, 0]))

        step = {}

        def one(i, carry):
            slot = lax.rem(i, 2)

            @pl.when(i == n_blk // 2)
            def _():
                pl.semaphore_wait(barrier, 10)
                step['y'] = stats_y(0)
                start(own_copies)

            @pl.when(i == 3 * n_blk // 4)
            def _():
                step['z'] = stats_z(0, step['y'])

            wait(loads(i))

            @pl.when(i >= 2)
            def _():
                wait(stores(i - 2))

            resid = rbuf[slot] + hbuf[slot].astype(F32)
            inv = lax.rsqrt(jnp.mean(resid * resid, axis=-1, keepdims=True) + NORM_EPS)
            h = (resid * inv * w_ref[...]).astype(BF16)
            hobuf[slot] = h
            for j in range(rb // LANES):
                row = (tgt_ref[pl.ds(i * (rb // LANES) + j, 1), :] - tp * vocab).astype(F32)
                col = jnp.broadcast_to(row, (LANES, LANES)).T
                ids[j * LANES:(j + 1) * LANES, :] = jnp.where((col >= 0) & (col < vocab), col, -1.0)
            mcbuf[slot, :, len(chunks) * LANES:] = ids[...]

            def finish(v):
                at = sum(chunks[:v])

                def some(r, carry):
                    first = pl.multiple_of(r * ROWS, ROWS)
                    rows = pl.ds(first, ROWS)
                    tgt = ids[rows, :].astype(jnp.int32)
                    tiles = [ge[kept(v, first, ROWS, k, LANES)] for k in range(0, chunks[v], LANES)]
                    pick = jnp.zeros((ROWS, LANES), F32)
                    for k, tile in enumerate(tiles):
                        pick = pick + jnp.where(lane == tgt - (at + k * LANES), tile, 0.0)
                    real = lane < vocab - (at + chunks[v] - LANES)
                    if at + chunks[v] > vocab:
                        top = functools.reduce(jnp.maximum, tiles[:-1] + [jnp.where(real, tiles[-1], -jnp.inf)])
                    else:
                        top = functools.reduce(jnp.maximum, tiles)
                    total = jnp.zeros((ROWS, LANES), F32)
                    for k, tile in enumerate(tiles):
                        e = jnp.exp(tile - top)
                        if at + (k + 1) * LANES > vocab:
                            e = jnp.where(real, e, 0.0)
                        ebuf[slot, rows, at + k * LANES:at + (k + 1) * LANES] = e
                        total = total + e
                    mcbuf[slot, rows, v * LANES:(v + 1) * LANES] = top
                    sums[v, rows, :] = total
                    picks[v, rows, :] = pick
                    return carry

                lax.fori_loop(0, rb // ROWS, some, 0, unroll=True)

            lane = lax.broadcasted_iota(jnp.int32, (ROWS, LANES), 1)
            at = 0
            for v, width in enumerate(chunks):
                for k in range(0, width, d):
                    part = min(d, width - k)
                    ge[kept(v, 0, rb, k, part)] = _dot(h, emb[at + k:at + k + part, :], 1, 1)
                if v:
                    finish(v - 1)
                at += width
            finish(len(chunks) - 1)
            maxes = [mcbuf[slot, :, v * LANES:(v + 1) * LANES] for v in range(len(chunks))]
            top = jnp.max(functools.reduce(jnp.maximum, maxes), axis=-1, keepdims=True)
            total = functools.reduce(jnp.add, [sums[v] * jnp.exp(m - top) for v, m in enumerate(maxes)])
            total = jnp.sum(total, axis=-1, keepdims=True)
            picked = jnp.sum(functools.reduce(jnp.add, [picks[v] for v in range(len(chunks))]), axis=-1, keepdims=True)
            lane = lax.broadcasted_iota(jnp.int32, (rb, LANES), 1)
            table = jnp.where(lane == 0, top, jnp.where(lane == 1, total, picked))
            sl = lax.div(i, n_blk // 2)
            for j in range(rb // LANES):
                tile = table[j * LANES:(j + 1) * LANES, :].T
                row = pl.ds((i - sl * (n_blk // 2)) * (rb // LANES) + j, 1)
                for k in range(3):
                    st[sl, k, row, :] = tile[k:k + 1, :]
            start(stores(i))

            @pl.when(i + 2 < n_blk)
            def _():
                start(loads(i + 2))

            return carry

        start(loads(0))
        start(loads(1))
        emb_copy.wait()
        lax.fori_loop(0, n_blk, one, 0)
        ahead['y'] = stats_y(1)
        wait(stores(n_blk - 2))
        wait(stores(n_blk - 1))
        stats_end(0, step['z'])

    def rows1(sl, kind, c, s):
        step = 1 + 2 * s
        chunk = lax.rem(place1(c) + jnp.where(kind == 0, 2, jnp.where(kind == 3, 0, step)), 4)
        half = jnp.where(kind == 1, 1 - s, s)
        return pl.multiple_of(sl * sl_rows + c * (sl_rows // 2) + chunk * ck + half * br, br)

    def r1_copy(sl, kind, c, s):
        rows = pl.ds(rows1(sl, kind, c, s), br)
        return remote(dh.at[rows, :], r1.at[sl, c, s, kind], r1_s.at[sl, c, s, kind], r1_r.at[sl, c, s, kind], axis1(c, 1 + 2 * s))

    def gradient_stage(ebuf, mcbuf, gbuf0, gbuf1, spread):
        gbufs = (gbuf0, gbuf1)
        row_id = lax.broadcasted_iota(jnp.int32, (LANES, LANES), 0)
        lane = lax.broadcasted_iota(jnp.int32, (ROWS, WIDE), 1)

        def piece(b, c, s):
            b = lax.rem(b, n_blk)
            return rows1(lax.div(b, 8), lax.rem(lax.div(b, 2), 4), c, s)

        def loads(b, c):
            out = []
            for s in PAIR:
                rows = pl.ds(piece(b, c, s), br)
                part = pl.ds(s * br, br)
                out.append(pltpu.make_async_copy(e_hbm.at[rows, :], ebuf.at[c, part, :], e_sem.at[c, s, 0]))
                out.append(pltpu.make_async_copy(mc_hbm.at[rows, :], mcbuf.at[c, part, :], e_sem.at[c, s, 1]))
            return out

        def stores(b, c):
            return [pltpu.make_async_copy(gbufs[c].at[pl.ds(s * br, br), :], g_hbm.at[pl.ds(piece(b, c, s), br), :], gw_sem.at[c, s, 0])
                    for s in PAIR]

        def prepare(b, c):
            for s in PAIR:
                at = lax.div(piece(b, c, s), LANES)
                cols = jnp.where(row_id == 0, fin[0, pl.ds(at, 1), :], fin[1, pl.ds(at, 1), :]).T
                part = slice(s * br, (s + 1) * br)
                for v in range(len(chunks)):
                    lanes = slice(v * LANES, (v + 1) * LANES)
                    spread[v, part, :] = jnp.exp(mcbuf[c, part, lanes] - cols[:, 0:1]) * cols[:, 1:2]

        def make_g(c, unroll=True):
            def some(r, carry):
                rows = pl.ds(pl.multiple_of(r * ROWS, ROWS), ROWS)
                tgt = mcbuf[c, rows, len(chunks) * LANES:].astype(jnp.int32)
                at = 0
                for v, width in enumerate(chunks):
                    scale = spread[v, rows, :]
                    for k in range(at, at + width, WIDE):
                        n = min(WIDE, at + width - k)
                        hit = lane[:, :n] == jnp.concatenate([tgt - k] * (n // LANES), axis=1)
                        g = ebuf[c, rows, k:k + n] * jnp.concatenate([scale] * (n // LANES), axis=1) - jnp.where(hit, inv_n, 0.0)
                        gbufs[c][rows, k:k + n] = g.astype(BF16)
                    at += width
                return carry

            lax.fori_loop(0, rb // ROWS, some, 0, unroll=unroll)

        def step(b, c):
            nb, nc = b + 1, 1 - c
            sl, kind = lax.div(b, 8), lax.rem(lax.div(b, 2), 4)
            wait(loads(nb, nc))

            @pl.when(nb >= 2)
            def _():
                wait(stores(nb - 2, nc))

            prepare(nb, nc)
            rows = [pl.ds(rows1(sl, kind, c, s), br) for s in PAIR]

            make_g(nc)
            value = _dot(gbufs[c][...], emb[...], 1, 0)
            for s in PAIR:
                dh[rows[s], :] = value[s * br:(s + 1) * br, :]

            @pl.when(nb < n_blk)
            def _():
                start(stores(nb, nc))

            @pl.when(nb + 2 <= n_blk)
            def _():
                start(loads(nb + 2, nc))

            @pl.when(kind < 2)
            def _():
                for s in PAIR:
                    r1_copy(sl, kind, c, s).start()

            @pl.when(kind == 2)
            def _():
                for s in PAIR:
                    r1_copy(sl, 0, c, s).wait_recv()
                    rows = pl.ds(rows1(sl, kind, c, s), br)
                    dh[rows, :] = dh[rows, :] + r1[sl, c, s, 0]
                    r1_copy(sl, 2, c, s).start()

        def pair(kk, carry):
            @pl.when(kk == 2)
            def _():
                stats_end(1, ahead['z'])

            @pl.when(kk == 6)
            def _():
                first_end(0)

            step(2 * kk, 0)
            step(2 * kk + 1, 1)
            return carry

        start(loads(0, 0))
        start(loads(1, 1))
        wait(loads(0, 0))
        prepare(0, 0)
        make_g(0, False)
        start(stores(0, 0))
        start(loads(2, 0))
        ahead['z'] = stats_z(1, ahead['y'])
        lax.fori_loop(0, n_blk // 2, pair, 0)
        wait(stores(n_blk - 1, 1))

    def rows2(sl, kind, c, s):
        chunk = lax.rem(place2(c) + (2 if kind == 0 else 0 if kind == 3 else STEP[s]), 4)
        half = 1 - s if kind == 1 else s
        return pl.multiple_of(sl * sl_rows + c * (sl_rows // 2) + place1(c) * ck + chunk * sb + half * b2, b2)

    def r2_copy(sl, kind, c, s):
        rows = pl.ds(rows2(sl, kind, c, s), b2)
        return remote(dh.at[rows, :], r2.at[sl, c, s, kind], r2_s.at[sl, c, s, kind], r2_r.at[sl, c, s, kind], axis2(c, STEP[s]))

    def first_end(sl):
        for c in PAIR:
            for s in PAIR:
                r1_copy(sl, 1, c, s).wait_recv()
                r1_copy(sl, 2, c, s).wait_recv()
        for c in PAIR:
            for half in PAIR:
                rows = pl.ds(rows1(sl, 3, c, half), br)
                dh[rows, :] = dh[rows, :] + r1[sl, c, half, 2] + r1[sl, c, 1 - half, 1]
        send([_Copy(r2_copy, sl, kind, c, s) for kind in (0, 1) for c in PAIR for s in PAIR])

    def second_relay(sl):
        for c in PAIR:
            for s in PAIR:
                r2_copy(sl, 0, c, s).wait_recv()
                rows = pl.ds(rows2(sl, 2, c, s), b2)
                dh[rows, :] = dh[rows, :] + r2[sl, c, s, 0]
                send([_Copy(r2_copy, sl, 2, c, s)])

    out_copies = []
    held = {}

    def ag2_copy(sl, c, s):
        at = pl.ds(own_rows[2 * sl + c], sb)
        return remote(dh.at[at, :], gr_out.at[at, :], ag2_s.at[sl, c, s, 0], ag2_r.at[sl, c, s, 0], axis2(c, STEP[s]))

    def own_copy(sl, c):
        at = pl.ds(own_rows[2 * sl + c], sb)
        return pltpu.make_async_copy(dh.at[at, :], gr_out.at[at, :], out_sem.at[2 * sl + c])

    def second_end(sl):
        for c in PAIR:
            for s in PAIR:
                r2_copy(sl, 1, c, s).wait_recv()
                r2_copy(sl, 2, c, s).wait_recv()
        w = w_ref[...]
        gw = jnp.zeros((1, d), F32)
        copies = []
        for c in PAIR:
            for half in PAIR:
                rows = pl.ds(rows2(sl, 3, c, half), b2)
                grad_h = dh[rows, :] + r2[sl, c, half, 2] + r2[sl, c, 1 - half, 1]
                part = pl.ds(half * b2, b2)
                resid = rown[sl, c, part, :] + hown[sl, c, part, :].astype(F32)
                inv = lax.rsqrt(jnp.mean(resid * resid, axis=-1, keepdims=True) + NORM_EPS)
                normed = resid * inv
                dn = grad_h * w
                dh[rows, :] = inv * (dn - normed * jnp.mean(dn * normed, axis=-1, keepdims=True))
                gw = gw + jnp.sum(grad_h * normed, axis=0, keepdims=True)
            copies += send([_Copy(ag2_copy, sl, c, s) for s in PAIR])
            out_copies.append(_Copy(own_copy, sl, c))
            out_copies[-1].start()
        gws[sl] = jnp.broadcast_to(gw, (8, d))
        return copies

    def own_chunk(sl, c, k):
        return pl.multiple_of(sl * sl_rows + c * (sl_rows // 2) + lax.rem(place1(c) + k, 4) * ck, ck)

    def fwd2_copy(sl, c, s):
        rows = pl.multiple_of(own_chunk(sl, c, 0) + lax.rem(place2(c) + STEP[1 - s], 4) * sb + s * b2, b2)
        part = gr_out.at[pl.ds(rows, b2), :]
        return remote(part, part, ag2_s.at[sl, c, s, 1], ag2_r.at[sl, c, s, 1], axis2(c, STEP[s]))

    def gather2(sl, copies):
        out = []
        for c in PAIR:
            for s in PAIR:
                copies[2 * c + s].wait_recv()
                out += send([_Copy(fwd2_copy, sl, c, s)])
        return out

    def ag1_copy(sl, c, s):
        part = gr_out.at[pl.ds(own_chunk(sl, c, 0), ck), :]
        return remote(part, part, ag1_s.at[sl, c, s, 0], ag1_r.at[sl, c, s, 0], axis1(c, STEP[s]))

    def gather1_start(sl, copies):
        out = []
        for c in PAIR:
            recv(copies[2 * c:2 * c + 2])
            out_copies[2 * sl + c].make().wait()
            out += send([_Copy(ag1_copy, sl, c, s) for s in PAIR])
        return out

    def fwd1_copy(sl, c, s):
        part = gr_out.at[pl.ds(pl.multiple_of(own_chunk(sl, c, STEP[1 - s]) + s * br, br), br), :]
        return remote(part, part, ag1_s.at[sl, c, s, 1], ag1_r.at[sl, c, s, 1], axis1(c, STEP[s]))

    def gather1(sl, copies):
        out = []
        for c in PAIR:
            for s in PAIR:
                copies[2 * c + s].wait_recv()
                out += send([_Copy(fwd1_copy, sl, c, s)])
        return out

    order = (2, 1, 3, 0)
    mine = pl.ds(pl.multiple_of(core * dx, LANES), dx)
    other = pl.ds(pl.multiple_of((1 - core) * dx, LANES), dx)

    def x_index(j):
        return lax.rem(x + order[j], 4)

    def x_base(j):
        return x_index(j) * (cx - ox)

    def c_copy(j):
        rows = pl.ds(pl.multiple_of(x_base(j), 8), cx)
        return remote(ge.at[j, rows, other], crecv.at[j], c_s.at[j], c_r.at[j], partner)

    def core_end(j):
        c_copy(j).wait_recv()

        def add(i, carry):
            rows = pl.ds(pl.multiple_of(x_base(j) + i * (cx // 4), 8), cx // 4)
            ge[j, rows, mine] = ge[j, rows, mine] + crecv[j, pl.ds(pl.multiple_of(i * (cx // 4), 8), cx // 4), :]
            return carry

        lax.fori_loop(0, 4, add, 0)

    def rows_x(kind, s):
        j = 0 if kind == 0 else 3 if kind == 3 else 1 + s
        half = 1 - s if kind == 1 else s
        return j, pl.ds(pl.multiple_of(x_base(j) + half * bx, 8), bx)

    def rx_copy(kind, s):
        j, rows = rows_x(kind, s)
        return remote(ge.at[j, rows, mine], rx.at[s, kind], rx_s.at[s, kind], rx_r.at[s, kind], at_x(STEP[s]))

    def small_copy(phase, k):
        place = (y, z, x, core)[phase]
        device = (at_tp(k, 0), at_tp(0, k), at_x(k), partner)[phase]
        return remote(smb.at[phase], smr.at[phase, place], sm_s.at[phase, k - 1], sm_r.at[phase, k - 1], device)

    def small_start(phase, value):
        smb[phase] = value
        smr[phase, (y, z, x, core)[phase]] = value
        return send([_Copy(small_copy, phase, k) for k in (OTHERS[:1] if phase == 3 else OTHERS)])

    def small_end(phase, copies):
        recv(copies)
        return functools.reduce(jnp.add, [smr[phase, k] for k in (PAIR if phase == 3 else range(RING))])

    def embed_stage(gbuf, hbuf):
        kb = n_tok // 4

        def loads(t):
            slot, rows = lax.rem(t, 2), pl.ds(pl.multiple_of(lax.rem(t, 4) * kb, kb), kb)
            first = lax.rem(x + jnp.where(t < 4, 2, jnp.where(t < 8, 1, jnp.where(t < 12, 3, 0))), 4)
            cols = pl.ds(pl.multiple_of(first * ox, LANES), wx)
            return (pltpu.make_async_copy(g_hbm.at[rows, cols], gbuf.at[slot], gin_sem.at[slot]),
                    pltpu.make_async_copy(h_hbm.at[rows, :], hbuf.at[slot], hin_sem.at[slot]))

        def chunk(j, middle):
            def one(k, carry):
                pl.when(k == 2)(middle)
                t = 4 * j + k
                slot = lax.rem(t, 2)
                wait(loads(t))
                ge[j] = ge[j] + _dot(gbuf[slot], hbuf[slot], 0, 0)

                @pl.when(t + 2 < 16)
                def _():
                    start(loads(t + 2))

                return carry

            ge[j] = jnp.zeros((wx, d), F32)
            lax.fori_loop(0, 4, one, 0)
            send([_Copy(c_copy, j)])

        def middle1():
            core_end(0)
            send([_Copy(rx_copy, 0, s) for s in PAIR])
            held[0] = second_end(0)

        def middle2():
            core_end(1)
            send([_Copy(rx_copy, 1, 0)])
            second_relay(1)

        def middle3():
            core_end(2)
            send([_Copy(rx_copy, 1, 1)])
            for s in PAIR:
                rx_copy(0, s).wait_recv()
                j, rows = rows_x(2, s)
                ge[j, rows, mine] = ge[j, rows, mine] + rx[s, 0]
                send([_Copy(rx_copy, 2, s)])
            held[1] = gather2(1, held[1])
            held['small'] = small_start(1, small_end(0, held['small']))

        start(loads(0))
        start(loads(1))
        wait(own_copies)
        chunk(0, functools.partial(second_relay, 0))
        chunk(1, middle1)
        held[0] = gather2(0, held[0])
        first_end(1)
        chunk(2, middle2)
        held[1] = second_end(1)
        row8 = lax.broadcasted_iota(jnp.int32, (8, d), 0)
        loss = losses[0, 0:1, 0:1] + losses[1, 0:1, 0:1]
        held['small'] = small_start(0, jnp.where(row8 == 0, gws[0] + gws[1], jnp.where(row8 == 1, loss, 0.0)))
        chunk(3, middle3)
        core_end(3)

    half_tile = pltpu.VMEM((len(chunks), rb, LANES), F32)
    tile = pltpu.VMEM((rb, LANES), F32)
    pl.run_scoped(
        logits_stage, pltpu.VMEM((2, rb, v_pad), F32), pltpu.VMEM((2, rb, mw), F32),
        pltpu.VMEM((2, rb, d), F32), pltpu.VMEM((2, rb, d), BF16), pltpu.VMEM((2, rb, d), BF16),
        half_tile, half_tile, tile)
    pl.run_scoped(
        gradient_stage, pltpu.VMEM((2, rb, v_pad), F32), pltpu.VMEM((2, rb, mw), F32),
        pltpu.VMEM((rb, v_pad), BF16), pltpu.VMEM((rb, v_pad), BF16),
        half_tile)
    pl.run_scoped(embed_stage, pltpu.VMEM((2, n_tok // 4, wx), BF16), pltpu.VMEM((2, n_tok // 4, d), BF16))

    held['small'] = small_start(2, small_end(1, held['small']))
    back0 = gather1_start(0, held[0])
    back1 = gather1_start(1, held[1])

    def out_rows(k, first=0, size=cx):
        return pl.ds(pl.multiple_of(lax.rem(x + k, 4) * cx + first, 8), size)

    for s in PAIR:
        rx_copy(1, s).wait_recv()
        rx_copy(2, s).wait_recv()
    for half in PAIR:
        j, rows = rows_x(3, half)
        ge[j, rows, mine] = ge[j, rows, mine] + rx[half, 2] + rx[1 - half, 1]
    src = ge.at[3, pl.ds(pl.multiple_of(x_base(3), 8), cx), mine]
    dst = ge_out.at[out_rows(0), mine]
    agx = send([_Copy(remote, src, dst, agx_s.at[s, 0], agx_r.at[s, 0], at_x(STEP[s])) for s in PAIR])
    agc = send([_Copy(remote, src, dst, agc_s.at[0], agc_r.at[0], partner)])
    ge_own = pltpu.make_async_copy(src, dst, out_sem.at[4])
    ge_own.start()
    last0 = gather1(0, back0)
    held['small'] = small_start(3, small_end(2, held['small']))
    last1 = gather1(1, back1)
    fwdx = []
    for s in PAIR:
        agx[s].wait_recv()
        part = ge_out.at[out_rows(STEP[1 - s], s * bx, bx), mine]
        fwdx += send([_Copy(remote, part, part, agx_s.at[s, 1], agx_r.at[s, 1], at_x(STEP[s]))])
        part = ge_out.at[out_rows(STEP[1 - s]), mine]
        agc += send([_Copy(remote, part, part, agc_s.at[1 + s], agc_r.at[1 + s], partner)])
    for s in PAIR:
        fwdx[s].wait_recv()
        part = ge_out.at[out_rows(2, s * bx, bx), mine]
        agc += send([_Copy(remote, part, part, agc_s.at[3 + s], agc_r.at[3 + s], partner)])
    small_out[...] = small_end(3, held['small'])
    recv(last0 + last1)

    for cp in agc:
        cp.wait_recv()
    ge_own.wait()

    def r1_sent(i, carry):
        r1_copy(lax.div(i, 12), lax.rem(lax.div(i, 4), 3), lax.rem(lax.div(i, 2), 2), lax.rem(i, 2)).wait_send()
        return carry

    lax.fori_loop(0, 24, r1_sent, 0)
    for cp in sent:
        cp.wait_send()


def solution(mesh, chunks=(1536, 1664)):
    def program(hidden, residual, targets, embedding, norm_w):
        inv_n = 1.0 / (hidden.shape[0] * hidden.shape[1])
        n_tp = mesh.shape['tp']

        def local_part(hid_loc, res_loc, tgt_loc, emb_loc, norm_vec):
            n_batch, n_seq, d = hid_loc.shape
            n_tok = n_batch * n_seq
            vocab = emb_loc.shape[0]
            v_pad = sum(chunks)
            br = n_tok // 32
            b2 = br // 4
            cx = v_pad // 4
            wx = (cx // LANES + 1) * LANES
            tiles = n_tok // (2 * LANES)
            dma = pltpu.SemaphoreType.DMA
            cube, kinds = (TWO, TWO, TWO), 3
            any_spec = pl.BlockSpec(memory_space=pl.ANY)
            vmem_spec = pl.BlockSpec(memory_space=pltpu.VMEM)
            shape = jax.ShapeDtypeStruct
            gr, ge, small, *_ = pl.pallas_call(
                functools.partial(_kernel, chunks, vocab, inv_n, n_tp),
                grid=(1,),
                in_specs=[vmem_spec, vmem_spec, pl.BlockSpec((16, d), lambda i: (vocab // 16, 0)), any_spec, any_spec, any_spec],
                out_specs=[any_spec, any_spec, vmem_spec, any_spec, any_spec, any_spec, any_spec],
                out_shape=[
                    shape((n_tok, d), F32), shape((v_pad, d), F32), shape((8, d), F32),
                    shape((n_tok, d), BF16), shape((n_tok, v_pad), F32), shape((n_tok, (len(chunks) + 1) * LANES), F32), shape((n_tok, v_pad), BF16),
                ],
                scratch_shapes=[
                    pltpu.VMEM((v_pad, d), BF16),
                    pltpu.VMEM((n_tok, d), F32),
                    pltpu.VMEM((RING, wx, d), F32),
                    pltpu.VMEM(cube + (kinds, br, d), F32),
                    pltpu.VMEM(cube + (kinds, b2, d), F32),
                    pltpu.VMEM((RING, cx, d // TWO), F32),
                    pltpu.VMEM((TWO, kinds, cx // TWO, d // TWO), F32),
                    pltpu.VMEM((TWO, kinds, tiles, LANES), F32),
                    pltpu.VMEM((TWO, RING, kinds, tiles, LANES), F32),
                    pltpu.VMEM((TWO, RING, kinds, tiles, LANES), F32),
                    pltpu.VMEM((TWO, kinds, tiles, LANES), F32),
                    pltpu.VMEM((TWO, TWO * tiles, LANES), F32),
                    pltpu.VMEM((TWO, TWO, TWO * b2, d), F32),
                    pltpu.VMEM((TWO, TWO, TWO * b2, d), BF16),
                    pltpu.VMEM((TWO, 8, LANES), F32),
                    pltpu.VMEM((TWO, 8, d), F32),
                    pltpu.VMEM((RING, 8, d), F32),
                    pltpu.VMEM((RING, RING, 8, d), F32),
                    dma, dma(cube), dma(cube), dma(cube), dma(cube), dma((TWO,)), dma((TWO,)), dma(cube),
                ] + [dma((TWO, RING))] * RING + [dma(cube + (kinds,))] * RING + [dma(cube + (TWO,))] * RING + [
                    dma((5,)), dma((RING,)), dma((RING,)), dma((TWO, kinds)), dma((TWO, kinds)), dma((TWO, TWO)), dma((TWO, TWO)),
                    dma((5,)), dma((5,)), dma((RING, kinds)), dma((RING, kinds)),
                ],
                compiler_params=pltpu.CompilerParams(collective_id=0, has_side_effects=True, vmem_limit_bytes=VMEM_BYTES),
                cost_estimate=pl.CostEstimate(flops=6 * n_tok * v_pad * d, bytes_accessed=8 * n_tok * v_pad, transcendentals=0),
            )(tgt_loc.reshape(n_tok // LANES, LANES), norm_vec.reshape(1, d), emb_loc, emb_loc, res_loc.reshape(n_tok, d), hid_loc.reshape(n_tok, d))
            return small[1, 0], gr.reshape(n_batch, n_seq, d), ge[:vocab], small[0]

        sharded = jax.shard_map(
            local_part, mesh=mesh,
            in_specs=(P('dp', None, None), P('dp', None, None), P('dp', None), P('tp', None), P(None)),
            out_specs=(P(), P('dp', None, None), P('tp', None), P(None)),
            check_vma=False)
        return sharded(hidden, residual, targets, embedding, norm_w)

    return program
```

```python
import functools

import jax
import jax.numpy as jnp
from jax import lax
from jax.experimental import pallas as pl
from jax.experimental.pallas import tpu as pltpu
from jax.sharding import PartitionSpec as P

NORM_EPS = 1e-5
LANES = 128
MESH = pl.DeviceIdType.MESH
ROWS = 16
WIDE = 512
PAIR = (0, 1)
OTHERS = (1, 2, 3)
TWO = 2
RING = 4
F32 = jnp.float32
BF16 = jnp.bfloat16
VMEM_BYTES = 67_043_328
STEP = (1, 3)


class _Copy:
    def __init__(self, make, *args):
        self.make = functools.partial(make, *args)

    def start(self):
        self.make().start()

    def wait_recv(self):
        self.make().wait_recv()

    def wait_send(self):
        self.make().wait_send()


def _dot(a, b, ca, cb):
    return lax.dot_general(a, b, (((ca,), (cb,)), ((), ())), preferred_element_type=F32)


def _kernel(chunks, vocab, inv_n, n_tp,
            tgt_ref, w_ref, tail_ref, emb_hbm, res_hbm, hid_hbm,
            gr_out, ge_out, small_out, h_hbm, e_hbm, mc_hbm, g_hbm,
            emb, dh, ge, r1, r2, crecv, rx, st, sy, sz, st2, fin, rown, hown, losses, gws, smb, smr,
            emb_sem, in_sem, l_sem, e_sem, gw_sem, gin_sem, hin_sem, own_sem, sy_s, sy_r, sz_s, sz_r, r1_s, r1_r, r2_s, r2_r,
            ag2_s, ag2_r, ag1_s, ag1_r, out_sem, c_s, c_r, rx_s, rx_r, agx_s, agx_r, agc_s, agc_r, sm_s, sm_r):
    n_tok, d = dh.shape
    v_pad = emb.shape[0]
    mw = (len(chunks) + 1) * LANES
    rb = 2 * LANES
    n_blk = n_tok // rb
    br = n_tok // 32
    b2 = br // 4
    ck, sb = 2 * br, 2 * b2
    dx = d // 2
    cx = v_pad // 4
    bx = cx // 2
    wx = ge.shape[1]
    ox = (cx // LANES) * LANES
    sl_rows = n_tok // 2

    tp = lax.axis_index('tp')
    dp = lax.axis_index('dp')
    y, z = lax.rem(tp, 4), lax.div(tp, 4)
    core, x = lax.rem(dp, 2), lax.div(dp, 2)

    def at_tp(dy, dz):
        return {'tp': lax.rem(z + dz, 4) * 4 + lax.rem(y + dy, 4)}

    def at_x(k):
        return {'dp': lax.rem(x + k, 4) * 2 + core}

    partner = {'dp': x * 2 + (1 - core)}

    def axis1(c, step):
        return at_tp(step * (1 - c), step * c)

    def axis2(c, step):
        return at_tp(step * c, step * (1 - c))

    def place1(c):
        return y * (1 - c) + z * c

    def place2(c):
        return z * (1 - c) + y * c

    def remote(src, dst, send, recv, device):
        return pltpu.make_async_remote_copy(src_ref=src, dst_ref=dst, send_sem=send, recv_sem=recv,
                                            device_id=device, device_id_type=MESH)

    def start(copies):
        for cp in copies:
            cp.start()

    def wait(copies):
        for cp in copies:
            cp.wait()

    sent = []

    def send(copies):
        start(copies)
        sent.extend(copies)
        return copies

    def recv(copies):
        for cp in copies:
            cp.wait_recv()

    barrier = pltpu.get_barrier_semaphore()
    for k in OTHERS:
        for device in (at_tp(k, 0), at_tp(0, k), at_x(k)):
            pl.semaphore_signal(barrier, inc=1, device_id=device, device_id_type=MESH)
    pl.semaphore_signal(barrier, inc=1, device_id=partner, device_id_type=MESH)

    whole = (vocab // 16) * 16
    tail = jnp.where(lax.broadcasted_iota(jnp.int32, (16, d), 0) < vocab - whole, tail_ref[...].astype(F32), 0.0)
    emb[whole:whole + 16, :] = tail.astype(BF16)
    emb[whole + 16:, :] = jnp.zeros((v_pad - whole - 16, d), BF16)
    emb_copy = pltpu.make_async_copy(emb_hbm.at[pl.ds(0, whole), :], emb.at[pl.ds(0, whole), :], emb_sem)
    emb_copy.start()
    own_rows, own_copies = [], []
    for sl in PAIR:
        for c in PAIR:
            rows = pl.multiple_of(sl * sl_rows + c * (sl_rows // 2) + place1(c) * ck + place2(c) * sb, sb)
            own_rows.append(rows)
            own_copies.append(pltpu.make_async_copy(res_hbm.at[pl.ds(rows, sb), :], rown.at[sl, c], own_sem.at[sl, c, 0]))
            own_copies.append(pltpu.make_async_copy(hid_hbm.at[pl.ds(rows, sb), :], hown.at[sl, c], own_sem.at[sl, c, 1]))

    def combine(parts):
        top = functools.reduce(jnp.maximum, [p[0] for p in parts])
        total = functools.reduce(jnp.add, [p[1] * jnp.exp(p[0] - top) for p in parts])
        return top, total, functools.reduce(jnp.add, [p[2] for p in parts])

    def stats_y(sl):
        return send([_Copy(lambda k: remote(st.at[sl], sy.at[sl, k], sy_s.at[sl, k], sy_r.at[sl, k], at_tp(k, 0)), k) for k in OTHERS])

    def stats_z(sl, copies):
        recv(copies)
        parts = combine([tuple(st[sl, k] for k in range(3))] + [tuple(sy[sl, j, k] for k in range(3)) for j in OTHERS])
        for k in range(3):
            st2[sl, k] = parts[k]
        return send([_Copy(lambda k: remote(st2.at[sl], sz.at[sl, k], sz_s.at[sl, k], sz_r.at[sl, k], at_tp(0, k)), k) for k in OTHERS])

    tiles_sl = sl_rows // LANES

    def stats_end(sl, copies):
        recv(copies)
        top, total, picked = combine([tuple(st2[sl, k] for k in range(3))] + [tuple(sz[sl, j, k] for k in range(3)) for j in OTHERS])
        fin[0, sl * tiles_sl:(sl + 1) * tiles_sl, :] = top
        fin[1, sl * tiles_sl:(sl + 1) * tiles_sl, :] = inv_n / total
        part = (top + jnp.log(total) - picked) * (inv_n / n_tp)
        losses[sl] = jnp.sum(jnp.sum(part, axis=0, keepdims=True), axis=1, keepdims=True) + jnp.zeros((8, LANES), F32)

    ahead = {}

    def block_rows(i):
        return pl.ds(pl.multiple_of(i * rb, rb), rb)

    def logits_stage(ebuf, mcbuf, rbuf, hbuf, hobuf, sums, picks, ids):
        def kept(v, first, size, k, width):
            return v, pl.ds((k // d) * rb + first, size), pl.ds(k % d, width)

        def loads(i):
            slot, rows = lax.rem(i, 2), block_rows(i)
            return (pltpu.make_async_copy(res_hbm.at[rows, :], rbuf.at[slot], in_sem.at[slot, 0, 0]),
                    pltpu.make_async_copy(hid_hbm.at[rows, :], hbuf.at[slot], in_sem.at[slot, 0, 1]))

        def stores(i):
            slot, rows = lax.rem(i, 2), block_rows(i)
            return (pltpu.make_async_copy(hobuf.at[slot], h_hbm.at[rows, :], l_sem.at[slot, 0, 0]),
                    pltpu.make_async_copy(ebuf.at[slot], e_hbm.at[rows, :], l_sem.at[slot, 0, 1]),
                    pltpu.make_async_copy(mcbuf.at[slot], mc_hbm.at[rows, :], l_sem.at[slot, 1, 0]))

        step = {}

        def one(i, carry):
            slot = lax.rem(i, 2)

            @pl.when(i == n_blk // 2)
            def _():
                pl.semaphore_wait(barrier, 10)
                step['y'] = stats_y(0)
                start(own_copies)

            @pl.when(i == 3 * n_blk // 4)
            def _():
                step['z'] = stats_z(0, step['y'])

            wait(loads(i))

            @pl.when(i >= 2)
            def _():
                wait(stores(i - 2))

            resid = rbuf[slot] + hbuf[slot].astype(F32)
            inv = lax.rsqrt(jnp.mean(resid * resid, axis=-1, keepdims=True) + NORM_EPS)
            h = (resid * inv * w_ref[...]).astype(BF16)
            hobuf[slot] = h
            for j in range(rb // LANES):
                row = (tgt_ref[pl.ds(i * (rb // LANES) + j, 1), :] - tp * vocab).astype(F32)
                col = jnp.broadcast_to(row, (LANES, LANES)).T
                ids[j * LANES:(j + 1) * LANES, :] = jnp.where((col >= 0) & (col < vocab), col, -1.0)
            mcbuf[slot, :, len(chunks) * LANES:] = ids[...]

            def finish(v):
                at = sum(chunks[:v])

                def some(r, carry):
                    first = pl.multiple_of(r * ROWS, ROWS)
                    rows = pl.ds(first, ROWS)
                    tgt = ids[rows, :].astype(jnp.int32)
                    tiles = [ge[kept(v, first, ROWS, k, LANES)] for k in range(0, chunks[v], LANES)]
                    pick = jnp.zeros((ROWS, LANES), F32)
                    for k, tile in enumerate(tiles):
                        pick = pick + jnp.where(lane == tgt - (at + k * LANES), tile, 0.0)
                    real = lane < vocab - (at + chunks[v] - LANES)
                    if at + chunks[v] > vocab:
                        top = functools.reduce(jnp.maximum, tiles[:-1] + [jnp.where(real, tiles[-1], -jnp.inf)])
                    else:
                        top = functools.reduce(jnp.maximum, tiles)
                    total = jnp.zeros((ROWS, LANES), F32)
                    for k, tile in enumerate(tiles):
                        e = jnp.exp(tile - top)
                        if at + (k + 1) * LANES > vocab:
                            e = jnp.where(real, e, 0.0)
                        ebuf[slot, rows, at + k * LANES:at + (k + 1) * LANES] = e
                        total = total + e
                    mcbuf[slot, rows, v * LANES:(v + 1) * LANES] = top
                    sums[v, rows, :] = total
                    picks[v, rows, :] = pick
                    return carry

                lax.fori_loop(0, rb // ROWS, some, 0, unroll=True)

            lane = lax.broadcasted_iota(jnp.int32, (ROWS, LANES), 1)
            at = 0
            for v, width in enumerate(chunks):
                for k in range(0, width, d):
                    part = min(d, width - k)
                    ge[kept(v, 0, rb, k, part)] = _dot(h, emb[at + k:at + k + part, :], 1, 1)
                if v:
                    finish(v - 1)
                at += width
            finish(len(chunks) - 1)
            maxes = [mcbuf[slot, :, v * LANES:(v + 1) * LANES] for v in range(len(chunks))]
            top = jnp.max(functools.reduce(jnp.maximum, maxes), axis=-1, keepdims=True)
            total = functools.reduce(jnp.add, [sums[v] * jnp.exp(m - top) for v, m in enumerate(maxes)])
            total = jnp.sum(total, axis=-1, keepdims=True)
            picked = jnp.sum(functools.reduce(jnp.add, [picks[v] for v in range(len(chunks))]), axis=-1, keepdims=True)
            lane = lax.broadcasted_iota(jnp.int32, (rb, LANES), 1)
            table = jnp.where(lane == 0, top, jnp.where(lane == 1, total, picked))
            sl = lax.div(i, n_blk // 2)
            for j in range(rb // LANES):
                tile = table[j * LANES:(j + 1) * LANES, :].T
                row = pl.ds((i - sl * (n_blk // 2)) * (rb // LANES) + j, 1)
                for k in range(3):
                    st[sl, k, row, :] = tile[k:k + 1, :]
            start(stores(i))

            @pl.when(i + 2 < n_blk)
            def _():
                start(loads(i + 2))

            return carry

        start(loads(0))
        start(loads(1))
        emb_copy.wait()
        lax.fori_loop(0, n_blk, one, 0)
        ahead['y'] = stats_y(1)
        wait(stores(n_blk - 2))
        wait(stores(n_blk - 1))
        stats_end(0, step['z'])

    def rows1(sl, kind, c, s):
        step = 1 + 2 * s
        chunk = lax.rem(place1(c) + jnp.where(kind == 0, 2, jnp.where(kind == 3, 0, step)), 4)
        half = jnp.where(kind == 1, 1 - s, s)
        return pl.multiple_of(sl * sl_rows + c * (sl_rows // 2) + chunk * ck + half * br, br)

    def r1_copy(sl, kind, c, s):
        rows = pl.ds(rows1(sl, kind, c, s), br)
        return remote(dh.at[rows, :], r1.at[sl, c, s, kind], r1_s.at[sl, c, s, kind], r1_r.at[sl, c, s, kind], axis1(c, 1 + 2 * s))

    def gradient_stage(ebuf, mcbuf, gbuf0, gbuf1, spread):
        gbufs = (gbuf0, gbuf1)
        row_id = lax.broadcasted_iota(jnp.int32, (LANES, LANES), 0)
        lane = lax.broadcasted_iota(jnp.int32, (ROWS, WIDE), 1)

        def piece(b, c, s):
            b = lax.rem(b, n_blk)
            return rows1(lax.div(b, 8), lax.rem(lax.div(b, 2), 4), c, s)

        def loads(b, c):
            out = []
            for s in PAIR:
                rows = pl.ds(piece(b, c, s), br)
                part = pl.ds(s * br, br)
                out.append(pltpu.make_async_copy(e_hbm.at[rows, :], ebuf.at[c, part, :], e_sem.at[c, s, 0]))
                out.append(pltpu.make_async_copy(mc_hbm.at[rows, :], mcbuf.at[c, part, :], e_sem.at[c, s, 1]))
            return out

        def stores(b, c):
            return [pltpu.make_async_copy(gbufs[c].at[pl.ds(s * br, br), :], g_hbm.at[pl.ds(piece(b, c, s), br), :], gw_sem.at[c, s, 0])
                    for s in PAIR]

        def prepare(b, c):
            for s in PAIR:
                at = lax.div(piece(b, c, s), LANES)
                cols = jnp.where(row_id == 0, fin[0, pl.ds(at, 1), :], fin[1, pl.ds(at, 1), :]).T
                part = slice(s * br, (s + 1) * br)
                for v in range(len(chunks)):
                    lanes = slice(v * LANES, (v + 1) * LANES)
                    spread[v, part, :] = jnp.exp(mcbuf[c, part, lanes] - cols[:, 0:1]) * cols[:, 1:2]

        def make_g(c, unroll=True):
            def some(r, carry):
                rows = pl.ds(pl.multiple_of(r * ROWS, ROWS), ROWS)
                tgt = mcbuf[c, rows, len(chunks) * LANES:].astype(jnp.int32)
                at = 0
                for v, width in enumerate(chunks):
                    scale = spread[v, rows, :]
                    for k in range(at, at + width, WIDE):
                        n = min(WIDE, at + width - k)
                        hit = lane[:, :n] == jnp.concatenate([tgt - k] * (n // LANES), axis=1)
                        g = ebuf[c, rows, k:k + n] * jnp.concatenate([scale] * (n // LANES), axis=1) - jnp.where(hit, inv_n, 0.0)
                        gbufs[c][rows, k:k + n] = g.astype(BF16)
                    at += width
                return carry

            lax.fori_loop(0, rb // ROWS, some, 0, unroll=unroll)

        def step(b, c):
            nb, nc = b + 1, 1 - c
            sl, kind = lax.div(b, 8), lax.rem(lax.div(b, 2), 4)
            wait(loads(nb, nc))

            @pl.when(nb >= 2)
            def _():
                wait(stores(nb - 2, nc))

            prepare(nb, nc)
            rows = [pl.ds(rows1(sl, kind, c, s), br) for s in PAIR]

            make_g(nc)
            value = _dot(gbufs[c][...], emb[...], 1, 0)
            for s in PAIR:
                dh[rows[s], :] = value[s * br:(s + 1) * br, :]

            @pl.when(nb < n_blk)
            def _():
                start(stores(nb, nc))

            @pl.when(nb + 2 <= n_blk)
            def _():
                start(loads(nb + 2, nc))

            @pl.when(kind < 2)
            def _():
                for s in PAIR:
                    r1_copy(sl, kind, c, s).start()

            @pl.when(kind == 2)
            def _():
                for s in PAIR:
                    r1_copy(sl, 0, c, s).wait_recv()
                    rows = pl.ds(rows1(sl, kind, c, s), br)
                    dh[rows, :] = dh[rows, :] + r1[sl, c, s, 0]
                    r1_copy(sl, 2, c, s).start()

        def pair(kk, carry):
            @pl.when(kk == 2)
            def _():
                stats_end(1, ahead['z'])

            @pl.when(kk == 6)
            def _():
                first_end(0)

            step(2 * kk, 0)
            step(2 * kk + 1, 1)
            return carry

        start(loads(0, 0))
        start(loads(1, 1))
        wait(loads(0, 0))
        prepare(0, 0)
        make_g(0, False)
        start(stores(0, 0))
        start(loads(2, 0))
        ahead['z'] = stats_z(1, ahead['y'])
        lax.fori_loop(0, n_blk // 2, pair, 0)
        wait(stores(n_blk - 1, 1))

    def rows2(sl, kind, c, s):
        chunk = lax.rem(place2(c) + (2 if kind == 0 else 0 if kind == 3 else STEP[s]), 4)
        half = 1 - s if kind == 1 else s
        return pl.multiple_of(sl * sl_rows + c * (sl_rows // 2) + place1(c) * ck + chunk * sb + half * b2, b2)

    def r2_copy(sl, kind, c, s):
        rows = pl.ds(rows2(sl, kind, c, s), b2)
        return remote(dh.at[rows, :], r2.at[sl, c, s, kind], r2_s.at[sl, c, s, kind], r2_r.at[sl, c, s, kind], axis2(c, STEP[s]))

    def first_end(sl):
        for c in PAIR:
            for s in PAIR:
                r1_copy(sl, 1, c, s).wait_recv()
                r1_copy(sl, 2, c, s).wait_recv()
        for c in PAIR:
            for half in PAIR:
                rows = pl.ds(rows1(sl, 3, c, half), br)
                dh[rows, :] = dh[rows, :] + r1[sl, c, half, 2] + r1[sl, c, 1 - half, 1]
        send([_Copy(r2_copy, sl, kind, c, s) for kind in (0, 1) for c in PAIR for s in PAIR])

    def second_relay(sl):
        for c in PAIR:
            for s in PAIR:
                r2_copy(sl, 0, c, s).wait_recv()
                rows = pl.ds(rows2(sl, 2, c, s), b2)
                dh[rows, :] = dh[rows, :] + r2[sl, c, s, 0]
                send([_Copy(r2_copy, sl, 2, c, s)])

    out_copies = []
    held = {}

    def ag2_copy(sl, c, s):
        at = pl.ds(own_rows[2 * sl + c], sb)
        return remote(dh.at[at, :], gr_out.at[at, :], ag2_s.at[sl, c, s, 0], ag2_r.at[sl, c, s, 0], axis2(c, STEP[s]))

    def own_copy(sl, c):
        at = pl.ds(own_rows[2 * sl + c], sb)
        return pltpu.make_async_copy(dh.at[at, :], gr_out.at[at, :], out_sem.at[2 * sl + c])

    def second_end(sl):
        for c in PAIR:
            for s in PAIR:
                r2_copy(sl, 1, c, s).wait_recv()
                r2_copy(sl, 2, c, s).wait_recv()
        w = w_ref[...]
        gw = jnp.zeros((1, d), F32)
        copies = []
        for c in PAIR:
            for half in PAIR:
                rows = pl.ds(rows2(sl, 3, c, half), b2)
                grad_h = dh[rows, :] + r2[sl, c, half, 2] + r2[sl, c, 1 - half, 1]
                part = pl.ds(half * b2, b2)
                resid = rown[sl, c, part, :] + hown[sl, c, part, :].astype(F32)
                inv = lax.rsqrt(jnp.mean(resid * resid, axis=-1, keepdims=True) + NORM_EPS)
                normed = resid * inv
                dn = grad_h * w
                dh[rows, :] = inv * (dn - normed * jnp.mean(dn * normed, axis=-1, keepdims=True))
                gw = gw + jnp.sum(grad_h * normed, axis=0, keepdims=True)
            copies += send([_Copy(ag2_copy, sl, c, s) for s in PAIR])
            out_copies.append(_Copy(own_copy, sl, c))
            out_copies[-1].start()
        gws[sl] = jnp.broadcast_to(gw, (8, d))
        return copies

    def own_chunk(sl, c, k):
        return pl.multiple_of(sl * sl_rows + c * (sl_rows // 2) + lax.rem(place1(c) + k, 4) * ck, ck)

    def fwd2_copy(sl, c, s):
        rows = pl.multiple_of(own_chunk(sl, c, 0) + lax.rem(place2(c) + STEP[1 - s], 4) * sb + s * b2, b2)
        part = gr_out.at[pl.ds(rows, b2), :]
        return remote(part, part, ag2_s.at[sl, c, s, 1], ag2_r.at[sl, c, s, 1], axis2(c, STEP[s]))

    def gather2(sl, copies):
        out = []
        for c in PAIR:
            for s in PAIR:
                copies[2 * c + s].wait_recv()
                out += send([_Copy(fwd2_copy, sl, c, s)])
        return out

    def ag1_copy(sl, c, s):
        part = gr_out.at[pl.ds(own_chunk(sl, c, 0), ck), :]
        return remote(part, part, ag1_s.at[sl, c, s, 0], ag1_r.at[sl, c, s, 0], axis1(c, STEP[s]))

    def gather1_start(sl, copies):
        out = []
        for c in PAIR:
            recv(copies[2 * c:2 * c + 2])
            out_copies[2 * sl + c].make().wait()
            out += send([_Copy(ag1_copy, sl, c, s) for s in PAIR])
        return out

    def fwd1_copy(sl, c, s):
        part = gr_out.at[pl.ds(pl.multiple_of(own_chunk(sl, c, STEP[1 - s]) + s * br, br), br), :]
        return remote(part, part, ag1_s.at[sl, c, s, 1], ag1_r.at[sl, c, s, 1], axis1(c, STEP[s]))

    def gather1(sl, copies):
        out = []
        for c in PAIR:
            for s in PAIR:
                copies[2 * c + s].wait_recv()
                out += send([_Copy(fwd1_copy, sl, c, s)])
        return out

    order = (2, 1, 3, 0)
    mine = pl.ds(pl.multiple_of(core * dx, LANES), dx)
    other = pl.ds(pl.multiple_of((1 - core) * dx, LANES), dx)

    def x_index(j):
        return lax.rem(x + order[j], 4)

    def x_base(j):
        return x_index(j) * (cx - ox)

    def c_copy(j):
        rows = pl.ds(pl.multiple_of(x_base(j), 8), cx)
        return remote(ge.at[j, rows, other], crecv.at[j], c_s.at[j], c_r.at[j], partner)

    def core_end(j):
        c_copy(j).wait_recv()

        def add(i, carry):
            rows = pl.ds(pl.multiple_of(x_base(j) + i * (cx // 4), 8), cx // 4)
            ge[j, rows, mine] = ge[j, rows, mine] + crecv[j, pl.ds(pl.multiple_of(i * (cx // 4), 8), cx // 4), :]
            return carry

        lax.fori_loop(0, 4, add, 0)

    def rows_x(kind, s):
        j = 0 if kind == 0 else 3 if kind == 3 else 1 + s
        half = 1 - s if kind == 1 else s
        return j, pl.ds(pl.multiple_of(x_base(j) + half * bx, 8), bx)

    def rx_copy(kind, s):
        j, rows = rows_x(kind, s)
        return remote(ge.at[j, rows, mine], rx.at[s, kind], rx_s.at[s, kind], rx_r.at[s, kind], at_x(STEP[s]))

    def small_copy(phase, k):
        place = (y, z, x, core)[phase]
        device = (at_tp(k, 0), at_tp(0, k), at_x(k), partner)[phase]
        return remote(smb.at[phase], smr.at[phase, place], sm_s.at[phase, k - 1], sm_r.at[phase, k - 1], device)

    def small_start(phase, value):
        smb[phase] = value
        smr[phase, (y, z, x, core)[phase]] = value
        return send([_Copy(small_copy, phase, k) for k in (OTHERS[:1] if phase == 3 else OTHERS)])

    def small_end(phase, copies):
        recv(copies)
        return functools.reduce(jnp.add, [smr[phase, k] for k in (PAIR if phase == 3 else range(RING))])

    def embed_stage(gbuf, hbuf):
        kb = n_tok // 4

        def loads(t):
            slot, rows = lax.rem(t, 2), pl.ds(pl.multiple_of(lax.rem(t, 4) * kb, kb), kb)
            first = lax.rem(x + jnp.where(t < 4, 2, jnp.where(t < 8, 1, jnp.where(t < 12, 3, 0))), 4)
            cols = pl.ds(pl.multiple_of(first * ox, LANES), wx)
            return (pltpu.make_async_copy(g_hbm.at[rows, cols], gbuf.at[slot], gin_sem.at[slot]),
                    pltpu.make_async_copy(h_hbm.at[rows, :], hbuf.at[slot], hin_sem.at[slot]))

        def chunk(j, middle):
            def one(k, carry):
                if middle:
                    pl.when(k == 2)(middle)
                t = 4 * j + k
                slot = lax.rem(t, 2)
                wait(loads(t))
                ge[j] = ge[j] + _dot(gbuf[slot], hbuf[slot], 0, 0)

                @pl.when(t + 2 < 16)
                def _():
                    start(loads(t + 2))

                return carry

            ge[j] = jnp.zeros((wx, d), F32)
            lax.fori_loop(0, 4, one, 0)
            send([_Copy(c_copy, j)])

        def middle1():
            core_end(0)
            send([_Copy(rx_copy, 0, s) for s in PAIR])

        def middle2():
            core_end(1)
            send([_Copy(rx_copy, 1, 0)])
            held[0] = gather2(0, held[0])

        def middle3():
            core_end(2)
            send([_Copy(rx_copy, 1, 1)])
            for s in PAIR:
                rx_copy(0, s).wait_recv()
                j, rows = rows_x(2, s)
                ge[j, rows, mine] = ge[j, rows, mine] + rx[s, 0]
                send([_Copy(rx_copy, 2, s)])
            held[1] = second_end(1)
            row8 = lax.broadcasted_iota(jnp.int32, (8, d), 0)
            loss = losses[0, 0:1, 0:1] + losses[1, 0:1, 0:1]
            held['small'] = small_start(0, jnp.where(row8 == 0, gws[0] + gws[1], jnp.where(row8 == 1, loss, 0.0)))

        start(loads(0))
        start(loads(1))
        wait(own_copies)
        chunk(0, None)
        second_relay(0)
        chunk(1, middle1)
        held[0] = second_end(0)
        first_end(1)
        chunk(2, middle2)
        second_relay(1)
        chunk(3, middle3)
        core_end(3)

    half_tile = pltpu.VMEM((len(chunks), rb, LANES), F32)
    tile = pltpu.VMEM((rb, LANES), F32)
    pl.run_scoped(
        logits_stage, pltpu.VMEM((2, rb, v_pad), F32), pltpu.VMEM((2, rb, mw), F32),
        pltpu.VMEM((2, rb, d), F32), pltpu.VMEM((2, rb, d), BF16), pltpu.VMEM((2, rb, d), BF16),
        half_tile, half_tile, tile)
    pl.run_scoped(
        gradient_stage, pltpu.VMEM((2, rb, v_pad), F32), pltpu.VMEM((2, rb, mw), F32),
        pltpu.VMEM((rb, v_pad), BF16), pltpu.VMEM((rb, v_pad), BF16),
        half_tile)
    pl.run_scoped(embed_stage, pltpu.VMEM((2, n_tok // 4, wx), BF16), pltpu.VMEM((2, n_tok // 4, d), BF16))

    held[1] = gather2(1, held[1])
    held['small'] = small_start(1, small_end(0, held['small']))
    back0 = gather1_start(0, held[0])
    held['small'] = small_start(2, small_end(1, held['small']))
    back1 = gather1_start(1, held[1])

    def out_rows(k, first=0, size=cx):
        return pl.ds(pl.multiple_of(lax.rem(x + k, 4) * cx + first, 8), size)

    for s in PAIR:
        rx_copy(1, s).wait_recv()
        rx_copy(2, s).wait_recv()
    for half in PAIR:
        j, rows = rows_x(3, half)
        ge[j, rows, mine] = ge[j, rows, mine] + rx[half, 2] + rx[1 - half, 1]
    def agx_copy(s, late):
        _, rows = rows_x(3, 1 - s if late else s)
        dst = ge_out.at[out_rows(0, (1 - s if late else s) * bx, bx), mine]
        return remote(ge.at[3, rows, mine], dst, agx_s.at[s, late], agx_r.at[s, late], at_x(STEP[s]))

    agx, agx_late = (send([_Copy(agx_copy, s, late) for s in PAIR]) for late in PAIR)
    src = ge.at[3, pl.ds(pl.multiple_of(x_base(3), 8), cx), mine]
    dst = ge_out.at[out_rows(0), mine]
    agc = send([_Copy(remote, src, dst, agc_s.at[0], agc_r.at[0], partner)])
    ge_own = pltpu.make_async_copy(src, dst, out_sem.at[4])
    ge_own.start()
    last0 = gather1(0, back0)
    held['small'] = small_start(3, small_end(2, held['small']))
    last1 = gather1(1, back1)
    fwdx = []
    for s in PAIR:
        agx[s].wait_recv()
        part = ge_out.at[out_rows(STEP[1 - s], s * bx, bx), mine]
        fwdx += send([_Copy(remote, part, part, agx_s.at[s, TWO], agx_r.at[s, TWO], at_x(STEP[s]))])
    for s in PAIR:
        agx_late[s].wait_recv()
        part = ge_out.at[out_rows(STEP[1 - s]), mine]
        agc += send([_Copy(remote, part, part, agc_s.at[1 + s], agc_r.at[1 + s], partner)])
    for s in PAIR:
        fwdx[s].wait_recv()
        part = ge_out.at[out_rows(2, s * bx, bx), mine]
        agc += send([_Copy(remote, part, part, agc_s.at[3 + s], agc_r.at[3 + s], partner)])
    small_out[...] = small_end(3, held['small'])
    recv(last0 + last1)

    for cp in agc:
        cp.wait_recv()
    ge_own.wait()

    def r1_sent(i, carry):
        r1_copy(lax.div(i, 12), lax.rem(lax.div(i, 4), 3), lax.rem(lax.div(i, 2), 2), lax.rem(i, 2)).wait_send()
        return carry

    lax.fori_loop(0, 24, r1_sent, 0)
    for cp in sent:
        cp.wait_send()


def solution(mesh, chunks=(1536, 1664)):
    def program(hidden, residual, targets, embedding, norm_w):
        inv_n = 1.0 / (hidden.shape[0] * hidden.shape[1])
        n_tp = mesh.shape['tp']

        def local_part(hid_loc, res_loc, tgt_loc, emb_loc, norm_vec):
            n_batch, n_seq, d = hid_loc.shape
            n_tok = n_batch * n_seq
            vocab = emb_loc.shape[0]
            v_pad = sum(chunks)
            br = n_tok // 32
            b2 = br // 4
            cx = v_pad // 4
            wx = (cx // LANES + 1) * LANES
            tiles = n_tok // (2 * LANES)
            dma = pltpu.SemaphoreType.DMA
            cube, kinds = (TWO, TWO, TWO), 3
            any_spec = pl.BlockSpec(memory_space=pl.ANY)
            vmem_spec = pl.BlockSpec(memory_space=pltpu.VMEM)
            shape = jax.ShapeDtypeStruct
            gr, ge, small, *_ = pl.pallas_call(
                functools.partial(_kernel, chunks, vocab, inv_n, n_tp),
                grid=(1,),
                in_specs=[vmem_spec, vmem_spec, pl.BlockSpec((16, d), lambda i: (vocab // 16, 0)), any_spec, any_spec, any_spec],
                out_specs=[any_spec, any_spec, vmem_spec, any_spec, any_spec, any_spec, any_spec],
                out_shape=[
                    shape((n_tok, d), F32), shape((v_pad, d), F32), shape((8, d), F32),
                    shape((n_tok, d), BF16), shape((n_tok, v_pad), F32), shape((n_tok, (len(chunks) + 1) * LANES), F32), shape((n_tok, v_pad), BF16),
                ],
                scratch_shapes=[
                    pltpu.VMEM((v_pad, d), BF16),
                    pltpu.VMEM((n_tok, d), F32),
                    pltpu.VMEM((RING, wx, d), F32),
                    pltpu.VMEM(cube + (kinds, br, d), F32),
                    pltpu.VMEM(cube + (kinds, b2, d), F32),
                    pltpu.VMEM((RING, cx, d // TWO), F32),
                    pltpu.VMEM((TWO, kinds, cx // TWO, d // TWO), F32),
                    pltpu.VMEM((TWO, kinds, tiles, LANES), F32),
                    pltpu.VMEM((TWO, RING, kinds, tiles, LANES), F32),
                    pltpu.VMEM((TWO, RING, kinds, tiles, LANES), F32),
                    pltpu.VMEM((TWO, kinds, tiles, LANES), F32),
                    pltpu.VMEM((TWO, TWO * tiles, LANES), F32),
                    pltpu.VMEM((TWO, TWO, TWO * b2, d), F32),
                    pltpu.VMEM((TWO, TWO, TWO * b2, d), BF16),
                    pltpu.VMEM((TWO, 8, LANES), F32),
                    pltpu.VMEM((TWO, 8, d), F32),
                    pltpu.VMEM((RING, 8, d), F32),
                    pltpu.VMEM((RING, RING, 8, d), F32),
                    dma, dma(cube), dma(cube), dma(cube), dma(cube), dma((TWO,)), dma((TWO,)), dma(cube),
                ] + [dma((TWO, RING))] * RING + [dma(cube + (kinds,))] * RING + [dma(cube + (TWO,))] * RING + [
                    dma((5,)), dma((RING,)), dma((RING,)), dma((TWO, kinds)), dma((TWO, kinds)), dma((TWO, kinds)), dma((TWO, kinds)),
                    dma((5,)), dma((5,)), dma((RING, kinds)), dma((RING, kinds)),
                ],
                compiler_params=pltpu.CompilerParams(collective_id=0, has_side_effects=True, vmem_limit_bytes=VMEM_BYTES),
                cost_estimate=pl.CostEstimate(flops=6 * n_tok * v_pad * d, bytes_accessed=8 * n_tok * v_pad, transcendentals=0),
            )(tgt_loc.reshape(n_tok // LANES, LANES), norm_vec.reshape(1, d), emb_loc, emb_loc, res_loc.reshape(n_tok, d), hid_loc.reshape(n_tok, d))
            return small[1, 0], gr.reshape(n_batch, n_seq, d), ge[:vocab], small[0]

        sharded = jax.shard_map(
            local_part, mesh=mesh,
            in_specs=(P('dp', None, None), P('dp', None, None), P('dp', None), P('tp', None), P(None)),
            out_specs=(P(), P('dp', None, None), P('tp', None), P(None)),
            check_vma=False)
        return sharded(hidden, residual, targets, embedding, norm_w)

    return program
```
